128 devices in a mesh: asset: 32 (over y, z, core), tm: 4 (over x).
Axes of the slice: x: 4, y: 4, z: 4, core: 2. Of those that a mesh axis runs over, the one named last changes fastest.
Arguments:
- values: float32 [4, 1024, 65536], P(None, 'tm', 'asset'), may hold values from -64 to 64
- listed_from: int32 [65536], P('asset'), may hold values from -1024 to 1023, as said below
- listed_until: int32 [65536], P('asset'), may hold values from -960 to 3070, as said below
Outputs:
- standardized: float32 [4, 1024, 65536], P(None, 'tm', 'asset')
The draws below stay inside these ranges and needn't reach their ends.
Inputs may be any that keep to these rules, and one draw needn't show every extreme that they name: listed_until[a] - listed_from[a] is at least 64. listed_until[a] - listed_from[a] is at least 64.
All inputs are finite; a program needn't handle non-finite values.
Results may differ from the reference program's by a relative error of at most 0.00005.
Values sent between devices are 32-bit elements; how exact they have to be, the bound alone decides.
No kernel may reach another device: no remote copies, remote signals or barrier semaphores. Data moves between devices by JAX's collectives and lax.ppermute only.
A program may use at most 128 MiB of HBM per device.

```python
import jax
import jax.numpy as jnp
from jax import lax

F = 4
WINDOW = 64
TIME = 1024
ASSETS = 65536


def listing_dates(key):
    base = jax.random.fold_in(key, 7)
    key_start, key_length = jax.random.split(base)
    first_stamp = jax.random.randint(key_start, (ASSETS,), -TIME, TIME, dtype=jnp.int32)
    length = jax.random.randint(key_length, (ASSETS,), WINDOW, 2 * TIME, dtype=jnp.int32)
    return (first_stamp, first_stamp + length)


def draw_listed_from(key, part):
    return listing_dates(key)[0]


def draw_listed_until(key, part):
    return listing_dates(key)[1]


def draw_values(key, part):
    base = jax.random.fold_in(key, 11)
    key_noise, key_scale, key_common, key_drift = jax.random.split(base, 4)
    noise_draw = jax.random.normal(key_noise, (F, TIME, ASSETS), jnp.float32)
    field_values = 8.0 * noise_draw
    return jnp.clip(field_values, -64.0, 64.0)


def setup_inputs(seed: int = 0) -> dict:
    arg_keys = jax.random.split(jax.random.key(seed), 4)
    values = draw_values(jax.random.fold_in(arg_keys[3], 71), 0)
    listed_from = draw_listed_from(jax.random.fold_in(arg_keys[3], 71), 0)
    listed_until = draw_listed_until(jax.random.fold_in(arg_keys[3], 71), 0)
    return {"values": values, "listed_from": listed_from, "listed_until": listed_until}


def standardize(field_values, weight, present):
    center = lax.optimization_barrier(jnp.sum(weight * field_values, axis=1)) / present
    deviate = (field_values - center[:, None]) * weight
    spread = lax.optimization_barrier(jnp.sum(deviate * deviate, axis=1)) / present
    return deviate / jnp.sqrt(spread + 0.1)[:, None]

def reference(values, listed_from, listed_until):
    stamps = jnp.arange(TIME, dtype=jnp.int32)[:, None]
    opened = listed_from[None, :]
    closed = listed_until[None, :]
    weight = ((stamps >= opened) & (stamps < closed)).astype(values.dtype)
    window_low = jnp.maximum(jnp.maximum(stamps - (WINDOW - 1), opened), 0)
    window_high = jnp.minimum(stamps, closed - 1)
    counted = jnp.maximum(window_high - window_low + 1, 1).astype(values.dtype)
    present = jnp.maximum(lax.optimization_barrier(jnp.sum(weight, axis=1)), 1.0)

    def one_field(field_values):
        window_sum = lax.reduce_window(field_values * weight, jnp.zeros((), field_values.dtype), lax.add, (WINDOW, 1), (1, 1), ((WINDOW - 1, 0), (0, 0)))
        rolling = window_sum / counted
        clipped = jnp.clip(standardize(rolling, weight, present), -3.0, 3.0)
        return standardize(clipped, weight, present)
    return lax.map(one_field, values)
```

```python
import functools

import jax
import jax.numpy as jnp
from jax import lax
from jax.experimental import pallas as pl
from jax.experimental.pallas import tpu as pltpu
from jax.sharding import PartitionSpec as P

WINDOW = 64
EPS = 0.1
LIMIT = 3.0
GROUP = 8
LANE = 128
LATE = 32
LATE_GROUPS = LATE // GROUP
SKIP_GROUPS = WINDOW // GROUP
VMEM = pl.BlockSpec(memory_space=pltpu.VMEM)
SMEM = pl.BlockSpec(memory_space=pltpu.SMEM)
ANY = pl.BlockSpec(memory_space=pl.ANY)
MIB = 1 << 20


def rows_of(g):
    return pl.ds(g * GROUP, GROUP)


def sublanes(width):
    return lax.broadcasted_iota(jnp.int32, (GROUP, width), 0)


def lanes_iota():
    return lax.broadcasted_iota(jnp.int32, (GROUP, LANE), 1)


def folded(x):
    total = x[:, :LANE]
    for at in range(LANE, x.shape[1], LANE):
        total = total + x[:, at : at + LANE]
    return total


def total_of(x):
    return jnp.sum(x, axis=1, keepdims=True)


def column(tile, lane, width):
    return jnp.broadcast_to(tile[:, lane : lane + 1], (GROUP, width))


def clipped_score(x, center, scale):
    return jnp.minimum(jnp.maximum((x - center) * scale, -LIMIT), LIMIT)


def moments(total, square, present):
    center = total / present
    spread = jnp.maximum(square / present - center * center, 0.0)
    return center, 1.0 / jnp.sqrt(spread + EPS)


def summed(gathered):
    total = gathered[0]
    for d in range(1, gathered.shape[0]):
        total = total + gathered[d]
    return total


def prefix_groups(groups, width):
    sub = sublanes(width)
    carried, out = None, []
    for x in groups:
        for s in (1, 2, 4):
            x = x + jnp.where(sub < s, 0.0, pltpu.roll(x, s, 0))
        if carried is not None:
            x = x + carried
        carried = jnp.broadcast_to(x[GROUP - 1 :, :], (GROUP, width))
        out.append(x)
    return out, carried


def first_pass(times, x_hbm, from_ref, until_ref, buf, inverse, pay, xs, sums, counts, sems):
    fields, rows, assets = x_hbm.shape
    own_groups = rows // GROUP
    groups = own_groups + LATE_GROUPS
    main = own_groups - SKIP_GROUPS
    chunks, _, _, width = xs.shape
    base, base_next = times[0], times[1]

    def fetch(c):
        lanes = pl.ds(pl.multiple_of(c * width, width), width)
        return pltpu.make_async_copy(x_hbm.at[:, :, lanes], xs.at[c], sems.at[c])

    for c in range(chunks):
        fetch(c).start()
    sums[...] = jnp.zeros_like(sums)
    counts[...] = jnp.zeros_like(counts)
    sub = sublanes(width)

    def chunk(c, carry):
        lanes = pl.ds(pl.multiple_of(c * width, width), width)
        opened = jnp.maximum(from_ref[:, lanes], 0)
        closed = until_ref[:, lanes]
        age = sub - opened
        left = closed - sub
        for g in range(groups):
            at = base + g * GROUP if g < own_groups else base_next + (g - own_groups) * GROUP
            seen = age + at
            listed = (seen >= 0) & (left > at)
            counted = jnp.clip(seen + 1, 1, WINDOW).astype(jnp.float32)
            inverse[rows_of(g), lanes] = jnp.where(listed, 1.0 / counted, 0.0)
            if g >= SKIP_GROUPS - LATE_GROUPS:
                which = g - (SKIP_GROUPS - LATE_GROUPS)
                counts[which] += folded(jnp.where(listed, 1.0, 0.0))
        fetch(c).wait()
        start = base + age

        def one_field(f, carry):
            last1 = last2 = last4 = last8 = None
            last16, last32 = [], []
            for g in range(groups):
                if g < own_groups:
                    x = jnp.where(start >= -g * GROUP, xs[c, f, rows_of(g), :], 0.0)
                else:
                    x = jnp.zeros((GROUP, width), jnp.float32)
                r = pltpu.roll(x, 1, 0)
                x = x + jnp.where(sub < 1, 0.0 if last1 is None else last1, r)
                last1 = r
                r = pltpu.roll(x, 2, 0)
                x = x + jnp.where(sub < 2, 0.0 if last2 is None else last2, r)
                last2 = r
                r = pltpu.roll(x, 4, 0)
                x = x + jnp.where(sub < 4, 0.0 if last4 is None else last4, r)
                last4 = r
                x16 = x if last8 is None else x + last8
                last8 = x
                x32 = x16 if len(last16) < 2 else x16 + last16[-2]
                last16 = last16[-1:] + [x16]
                x64 = x32 if len(last32) < 4 else x32 + last32[-4]
                last32 = last32[-3:] + [x32]
                if SKIP_GROUPS <= g < own_groups:
                    x64 = x64 * inverse[rows_of(g), lanes]
                    sums[0, f, g - SKIP_GROUPS] += folded(x64)
                    sums[1, f, g - SKIP_GROUPS] += folded(x64 * x64)
                buf[f, rows_of(g), lanes] = x64
            return carry

        lax.fori_loop(0, fields, one_field, 0)
        return carry

    lax.fori_loop(0, chunks, chunk, 0)
    lane = lanes_iota()
    tiles = [jnp.zeros((GROUP, LANE), jnp.float32) for _ in range(2)]
    for stat in range(2):
        for f in range(fields):
            for g in range(main):
                tiles[stat] = jnp.where(lane == f * main + g, total_of(sums[stat, f, g]), tiles[stat])
    first = fields * main
    for g in range(main):
        tiles[0] = jnp.where(lane == first + g, total_of(counts[LATE_GROUPS + g]), tiles[0])
    for side in range(2):
        for g in range(LATE_GROUPS):
            spot = lane - (first + side * fields * LATE_GROUPS)
            here = (spot >= 0) & (spot < fields * LATE_GROUPS) & (lax.rem(spot, LATE_GROUPS) == g)
            at = g if side == 0 else LATE_GROUPS + main + g
            tiles[1] = jnp.where(here, total_of(counts[at]), tiles[1])
    for d in range(pay.shape[0]):
        pay[d, :GROUP, :] = tiles[0]
        pay[d, GROUP:, :] = tiles[1]


def second_pass(gathered, buf, inverse, stats, part):
    fields, _, assets = buf.shape
    main = (inverse.shape[0] - LATE) // GROUP - SKIP_GROUPS
    first = fields * main
    total = summed(gathered)
    t0, t1 = total[:GROUP], total[GROUP:]
    lane = lanes_iota()
    present = t1
    for f in range(fields):
        moved = pltpu.roll(t0, (f * main - first) % LANE, 1)
        present = jnp.where((lane >= f * main) & (lane < (f + 1) * main), moved, present)
    present = jnp.maximum(present, 1.0)
    center, scale = moments(t0, t1, present)
    stats[0], stats[1], stats[2] = center, scale, present
    width = 4 * LANE
    tiles = [jnp.zeros((GROUP, LANE), jnp.float32) for _ in range(2)]
    for g in range(main):
        rows = rows_of(g + SKIP_GROUPS)
        cs = [column(center, f * main + g, width) for f in range(fields)]
        ss = [column(scale, f * main + g, width) for f in range(fields)]

        def tile(i, acc):
            lanes = pl.ds(pl.multiple_of(i * width, width), width)
            listed = inverse[rows, lanes] > 0.0
            acc = list(acc)
            for f in range(fields):
                z = clipped_score(buf[f, rows, lanes], cs[f], ss[f])
                z = jnp.where(listed, z, 0.0)
                acc[f] = acc[f] + folded(z)
                acc[fields + f] = acc[fields + f] + folded(z * z)
            return tuple(acc)

        zero = jnp.zeros((GROUP, LANE), jnp.float32)
        acc = lax.fori_loop(0, assets // width, tile, (zero,) * (2 * fields))
        for f in range(fields):
            for stat in range(2):
                tiles[stat] = jnp.where(
                    lane == f * main + g, total_of(acc[stat * fields + f]), tiles[stat]
                )
    part[:GROUP, :] = tiles[0]
    part[GROUP:, :] = tiles[1]


def late_first_pass(times, buf, tail, head, from_ref, inverse, part, late, whole, pay):
    fields, _, assets = buf.shape
    rows = inverse.shape[0] - LATE
    base, base_next = times[0], times[1]
    follows = jnp.where(base_next > 0, 1.0, 0.0)
    width = LANE
    sub = sublanes(width)
    lane = lanes_iota()
    first = LANE - 2 * fields * LATE_GROUPS
    tiles = [part[:GROUP, :], part[GROUP:, :]]
    for f in range(fields):

        def tile(i, acc):
            lanes = pl.ds(pl.multiple_of(i * width, width), width)
            age = sub - jnp.maximum(from_ref[:, lanes], 0)
            acc = list(acc)
            for side, ref, at in ((0, tail, base - LATE), (1, head, base_next)):
                start = age + at
                masked = [
                    jnp.where(start >= -g * GROUP, ref[f, rows_of(g), lanes], 0.0)
                    for g in range(LATE_GROUPS)
                ]
                running, last = prefix_groups(masked, width)
                if side == 0:
                    whole[f, :, lanes] = last
                for g in range(LATE_GROUPS):
                    if side == 0:
                        where = rows_of(LATE_GROUPS + g)
                        r = buf[f, where, lanes] + (last - running[g])
                    else:
                        where = rows_of(rows // GROUP + g)
                        r = buf[f, where, lanes] * follows + running[g]
                    r = r * inverse[where, lanes]
                    late[f, rows_of(side * LATE_GROUPS + g), lanes] = r
                    k = side * LATE_GROUPS + g
                    acc[k] = acc[k] + r
                    acc[2 * LATE_GROUPS + k] = acc[2 * LATE_GROUPS + k] + r * r
            return tuple(acc)

        zero = jnp.zeros((GROUP, LANE), jnp.float32)
        acc = lax.fori_loop(0, assets // width, tile, (zero,) * (4 * LATE_GROUPS))
        for side in range(2):
            for g in range(LATE_GROUPS):
                spot = first + (side * fields + f) * LATE_GROUPS + g
                for stat in range(2):
                    value = total_of(acc[(stat * 2 + side) * LATE_GROUPS + g])
                    tiles[stat] = jnp.where(lane == spot, value, tiles[stat])
    for d in range(pay.shape[0]):
        pay[d, :GROUP, :] = tiles[0]
        pay[d, GROUP:, :] = tiles[1]


def late_second_pass(gathered, stats, late, inverse, level, pay):
    fields, _, assets = late.shape
    rows = inverse.shape[0] - LATE
    total = summed(gathered)
    center, scale = moments(total[:GROUP], total[GROUP:], stats[2])
    level[0], level[1] = center, scale
    width = 4 * LANE
    first = LANE - 2 * fields * LATE_GROUPS
    lane = lanes_iota()
    out = jnp.zeros((GROUP, LANE), jnp.float32)
    for side in range(2):
        for g in range(LATE_GROUPS):
            spots = [first + (side * fields + f) * LATE_GROUPS + g for f in range(fields)]
            cs = [column(center, spot, width) for spot in spots]
            ss = [column(scale, spot, width) for spot in spots]
            where = rows_of(LATE_GROUPS + g if side == 0 else rows // GROUP + g)
            mine = rows_of(side * LATE_GROUPS + g)

            def tile(i, acc):
                lanes = pl.ds(pl.multiple_of(i * width, width), width)
                listed = inverse[where, lanes] > 0.0
                acc = list(acc)
                for f in range(fields):
                    z = clipped_score(late[f, mine, lanes], cs[f], ss[f])
                    z = jnp.where(listed, z, 0.0)
                    acc[f] = acc[f] + folded(z)
                    acc[fields + f] = acc[fields + f] + folded(z * z)
                return tuple(acc)

            zero = jnp.zeros((GROUP, LANE), jnp.float32)
            acc = lax.fori_loop(0, assets // width, tile, (zero,) * (2 * fields))
            back = LANE - first
            for f in range(fields):
                out = jnp.where(lane == spots[f], total_of(acc[f]), out)
                out = jnp.where(lane == spots[f] - back, total_of(acc[fields + f]), out)
    for d in range(pay.shape[0]):
        pay[d] = out


def final_rows(f, where, source, mine, inverse, stage, put, cols, assets):
    width = 4 * LANE
    c1, s1, c2, s2 = cols

    def tile(i, carry):
        lanes = pl.ds(pl.multiple_of(i * width, width), width)
        z = clipped_score(source[f, mine, lanes], c1, s1)
        z = (z - c2) * s2
        stage[f, put, lanes] = jnp.where(inverse[where, lanes] > 0.0, z, 0.0)
        return carry

    lax.fori_loop(0, assets // width, tile, 0)


def main_final_pass(buf, inverse, stats, level, out, stage, sems):
    fields, rows, assets = out.shape
    main = rows // GROUP - SKIP_GROUPS
    width = 4 * LANE
    c1, s1, c2, s2 = stats[0], stats[1], level[0], level[1]
    copies = []
    for f in range(fields):
        for g in range(main):
            spot = f * main + g
            where = rows_of(g + SKIP_GROUPS)
            cols = [column(t, spot, width) for t in (c1, s1, c2, s2)]
            final_rows(f, where, buf, where, inverse, stage, rows_of(g), cols, assets)
        copy = pltpu.make_async_copy(
            stage.at[f], out.at[f, pl.ds(WINDOW, rows - WINDOW), :], sems.at[f]
        )
        copy.start()
        copies.append(copy)
    for copy in copies:
        copy.wait()


def send_pass(gathered, stats, level, level4, pay):
    total = summed(gathered)
    back = 32
    square = pltpu.roll(total, back, 1)
    center, scale = moments(total, square, stats[2])
    level4[0], level4[1] = center, scale
    lane = lanes_iota()
    out = jnp.zeros((GROUP, LANE), jnp.float32)
    for i, t in enumerate((level[0], level[1], center, scale)):
        moved = pltpu.roll(t, 16 * (i + 1), 1)
        out = jnp.where((lane >= 16 * i) & (lane < 16 * (i + 1)), moved, out)
    pay[...] = out


def late_final_pass(late, inverse, level, level4, prior, out, stage, sems):
    fields, _, assets = late.shape
    width = 4 * LANE
    first = LANE - 2 * fields * LATE_GROUPS
    copies = []
    for f in range(fields):
        for g in range(LATE_GROUPS):
            spot = first + f * LATE_GROUPS + g
            tiles = (level[0], level[1], level4[0], level4[1])
            cols = [column(t, spot, width) for t in tiles]
            where = rows_of(LATE_GROUPS + g)
            final_rows(f, where, late, rows_of(g), inverse, stage, rows_of(g), cols, assets)
        copy = pltpu.make_async_copy(stage.at[f], out.at[f, pl.ds(LATE, LATE), :], sems.at[f])
        copy.start()
        copies.append(copy)
    for copy in copies:
        copy.wait()


def head_final_pass(times, buf, tail, whole, from_ref, inverse, sent, prior, out, stage, sems):
    fields, _, assets = buf.shape
    base = times[0]
    width = 2 * LANE
    sub = sublanes(width)
    levels = sent[...]
    copies = []
    for f in range(fields):
        cols = [
            [column(levels, 16 * i + f * LATE_GROUPS + g, width) for i in range(4)]
            for g in range(LATE_GROUPS)
        ]

        def tile(i, carry):
            lanes = pl.ds(pl.multiple_of(i * width, width), width)
            start = sub - jnp.maximum(from_ref[:, lanes], 0) + (base - WINDOW)
            masked = [
                jnp.where(start >= -g * GROUP, tail[f, rows_of(g), lanes], 0.0)
                for g in range(LATE_GROUPS)
            ]
            running, last = prefix_groups(masked, width)
            last = last + whole[f, :, lanes]
            for g in range(LATE_GROUPS):
                c1, s1, c2, s2 = cols[g]
                weight = inverse[rows_of(g), lanes]
                r = (buf[f, rows_of(g), lanes] + (last - running[g])) * weight
                z = (clipped_score(r, c1, s1) - c2) * s2
                stage[f, rows_of(g), lanes] = jnp.where(weight > 0.0, z, 0.0)
            return carry

        lax.fori_loop(0, assets // width, tile, 0)
        copy = pltpu.make_async_copy(stage.at[f], out.at[f, pl.ds(0, LATE), :], sems.at[f])
        copy.start()
        copies.append(copy)
    for copy in copies:
        copy.wait()


def shape(*dims):
    return jax.ShapeDtypeStruct(dims, jnp.float32)


def call(body, name, ins, outs, out_specs, scratch=(), limit=8, flops=0, aliases=None):
    return pl.pallas_call(
        body,
        name=name,
        out_shape=outs,
        in_specs=ins,
        out_specs=out_specs,
        scratch_shapes=list(scratch),
        input_output_aliases=aliases or {},
        compiler_params=pltpu.CompilerParams(vmem_limit_bytes=limit * MIB),
        cost_estimate=pl.CostEstimate(flops=flops, bytes_accessed=0, transcendentals=0),
    )


def per_device(values, listed_from, listed_until):
    fields, rows, assets = values.shape
    n = lax.axis_size("asset")
    blocks = lax.axis_size("tm")
    block = lax.axis_index("tm")
    forward = [(i, i + 1) for i in range(blocks - 1)]
    ring = [(i, (i + 1) % blocks) for i in range(blocks)]
    back = [((i + 1) % blocks, i) for i in range(blocks)]
    tail_near = lax.ppermute(values[:, rows - LATE :], "tm", forward)
    head = lax.ppermute(values[:, :LATE], "tm", back)
    tail_far = lax.ppermute(values[:, rows - WINDOW : rows - LATE], "tm", forward)
    times = jnp.stack([block * rows, lax.rem(block + 1, blocks) * rows]).astype(jnp.int32)
    opened, closed = listed_from.reshape(1, assets), listed_until.reshape(1, assets)
    main = rows // GROUP - SKIP_GROUPS
    width = 2 * LANE
    chunks = assets // width
    tile = shape(GROUP, LANE)
    pair = shape(2, GROUP, LANE)
    exchange = functools.partial(
        lax.all_to_all, axis_name="asset", split_axis=0, concat_axis=0, tiled=True
    )
    work = fields * rows * assets

    buf, inverse, pay = call(
        first_pass, "first_pass", [SMEM, ANY, VMEM, VMEM],
        (shape(fields, rows + LATE, assets), shape(rows + LATE, assets), shape(n, 2 * GROUP, LANE)),
        (VMEM, VMEM, VMEM),
        [
            pltpu.VMEM((chunks, fields, rows, width), jnp.float32),
            pltpu.VMEM((2, fields, main, GROUP, LANE), jnp.float32),
            pltpu.VMEM((main + 2 * LATE_GROUPS, GROUP, LANE), jnp.float32),
            pltpu.SemaphoreType.DMA((chunks,)),
        ],
        limit=26, flops=20 * work,
    )(times, values, opened, closed)
    gathered = exchange(pay)
    stats, part = call(
        second_pass, "second_pass", [VMEM] * 3,
        (shape(3, GROUP, LANE), shape(2 * GROUP, LANE)), (VMEM, VMEM), limit=16, flops=10 * work,
    )(gathered, buf, inverse)
    late, whole, pay = call(
        late_first_pass, "late_first_pass", [SMEM] + [VMEM] * 6,
        (shape(fields, 2 * LATE, assets), shape(fields, GROUP, assets), shape(n, 2 * GROUP, LANE)),
        (VMEM, VMEM, VMEM), limit=20, flops=5 * work,
    )(times, buf, tail_near, head, opened, inverse, part)
    gathered = exchange(pay)
    level, pay = call(
        late_second_pass, "late_second_pass", [VMEM] * 4,
        (pair, shape(n, GROUP, LANE)), (VMEM, VMEM), limit=16, flops=3 * work,
    )(gathered, stats, late, inverse)
    gathered = exchange(pay)
    out = call(
        main_final_pass, "main_final_pass", [VMEM] * 4,
        shape(fields, rows, assets), ANY,
        [
            pltpu.VMEM((fields, rows - WINDOW, assets), jnp.float32),
            pltpu.SemaphoreType.DMA((fields,)),
        ],
        limit=20, flops=10 * work,
    )(buf, inverse, stats, level)
    level4, pay = call(
        send_pass, "send_pass", [VMEM] * 3, (pair, tile), (VMEM, VMEM), flops=work // 100,
    )(gathered, stats, level)
    sent = lax.ppermute(pay, "tm", ring)
    stage = [
        pltpu.VMEM((fields, LATE, assets), jnp.float32),
        pltpu.SemaphoreType.DMA((fields,)),
    ]
    out = call(
        late_final_pass, "late_final_pass", [VMEM] * 4 + [ANY],
        shape(fields, rows, assets), ANY, stage, limit=16, flops=2 * work, aliases={4: 0},
    )(late, inverse, level, level4, out)
    return call(
        head_final_pass, "head_final_pass", [SMEM] + [VMEM] * 6 + [ANY],
        shape(fields, rows, assets), ANY, stage, limit=16, flops=2 * work, aliases={7: 0},
    )(times, buf, tail_far, whole, opened, inverse, sent, out)


def solution(mesh):
    in_specs = (P(None, "tm", "asset"), P("asset"), P("asset"))
    out_specs = P(None, "tm", "asset")
    return jax.shard_map(
        per_device, mesh=mesh, in_specs=in_specs, out_specs=out_specs, check_vma=False
    )
```

```python
import functools

import jax
import jax.numpy as jnp
from jax import lax
from jax.experimental import pallas as pl
from jax.experimental.pallas import tpu as pltpu
from jax.sharding import PartitionSpec as P

WINDOW = 64
EPS = 0.1
LIMIT = 3.0
GROUP = 8
LANE = 128
LATE = 32
LATE_GROUPS = LATE // GROUP
SKIP_GROUPS = WINDOW // GROUP
VMEM = pl.BlockSpec(memory_space=pltpu.VMEM)
HBM = pl.BlockSpec(memory_space=pltpu.HBM)
MIB = 1 << 20


def rows_of(g):
    return pl.ds(g * GROUP, GROUP)


def block_starts(rows):
    block, blocks = lax.axis_index("tm"), lax.axis_size("tm")
    return block * rows, lax.rem(block + 1, blocks) * rows


def sublanes(width):
    return lax.broadcasted_iota(jnp.int32, (GROUP, width), 0)


def lanes_iota():
    return lax.broadcasted_iota(jnp.int32, (GROUP, LANE), 1)


def folded(x):
    total = x[:, :LANE]
    for at in range(LANE, x.shape[1], LANE):
        total = total + x[:, at : at + LANE]
    return total


def total_of(x):
    return jnp.sum(x, axis=1, keepdims=True)


def column(tile, lane, width):
    return jnp.broadcast_to(tile[:, lane : lane + 1], (GROUP, width))


def clipped_score(x, center, scale):
    return jnp.minimum(jnp.maximum((x - center) * scale, -LIMIT), LIMIT)


def moments(total, square, present):
    center = total / present
    spread = jnp.maximum(square / present - center * center, 0.0)
    return center, 1.0 / jnp.sqrt(spread + EPS)


def summed(gathered):
    total = gathered[0]
    for d in range(1, gathered.shape[0]):
        total = total + gathered[d]
    return total


def prefix_groups(groups, width):
    sub = sublanes(width)
    carried, out = None, []
    for x in groups:
        for s in (1, 2, 4):
            x = x + jnp.where(sub < s, 0.0, pltpu.roll(x, s, 0))
        if carried is not None:
            x = x + carried
        carried = jnp.broadcast_to(x[GROUP - 1 :, :], (GROUP, width))
        out.append(x)
    return out, carried


def load(x_hbm, near, head, x_ref, sems):
    rows = x_hbm.shape[1]
    copies = [
        pltpu.make_async_copy(x_hbm.at[:, pl.ds(rows - LATE, LATE), :], near, sems.at[0]),
        pltpu.make_async_copy(x_hbm.at[:, pl.ds(0, LATE), :], head, sems.at[1]),
        pltpu.make_async_copy(x_hbm, x_ref, sems.at[2]),
    ]
    for copy in copies:
        copy.start()
    for copy in copies:
        copy.wait()


def first_pass(
    x_ref, from_hbm, until_hbm,
    buf, inverse, pay, far, from_ref, until_ref, sums, counts, date_sems,
):
    fields, rows, assets = x_ref.shape
    own_groups = rows // GROUP
    groups = own_groups + LATE_GROUPS
    main = own_groups - SKIP_GROUPS
    width = 2 * LANE
    base, base_next = block_starts(rows)
    dates = [
        pltpu.make_async_copy(from_hbm, from_ref, date_sems.at[0]),
        pltpu.make_async_copy(until_hbm, until_ref, date_sems.at[1]),
    ]
    for copy in dates:
        copy.start()
    sums[...] = jnp.zeros_like(sums)
    counts[...] = jnp.zeros_like(counts)
    sub = sublanes(width)
    for copy in dates:
        copy.wait()

    def chunk(c, carry):
        lanes = pl.ds(pl.multiple_of(c * width, width), width)
        opened = jnp.maximum(from_ref[:, lanes], 0)
        closed = until_ref[:, lanes]
        age = sub - opened
        left = closed - sub
        for g in range(groups):
            at = base + g * GROUP if g < own_groups else base_next + (g - own_groups) * GROUP
            seen = age + at
            listed = (seen >= 0) & (left > at)
            counted = jnp.clip(seen + 1, 1, WINDOW).astype(jnp.float32)
            inverse[rows_of(g), lanes] = jnp.where(listed, 1.0 / counted, 0.0)
            if g >= SKIP_GROUPS - LATE_GROUPS:
                which = g - (SKIP_GROUPS - LATE_GROUPS)
                counts[which] += folded(jnp.where(listed, 1.0, 0.0))
        start = base + age

        def one_field(f, carry):
            last1 = last2 = last4 = last8 = None
            last16, last32 = [], []
            for g in range(groups):
                if own_groups - SKIP_GROUPS <= g < own_groups - LATE_GROUPS:
                    to = rows_of(g - (own_groups - SKIP_GROUPS))
                    far[f, to, lanes] = x_ref[f, rows_of(g), lanes]
                if g < own_groups:
                    x = jnp.where(start >= -g * GROUP, x_ref[f, rows_of(g), lanes], 0.0)
                else:
                    x = jnp.zeros((GROUP, width), jnp.float32)
                r = pltpu.roll(x, 1, 0)
                x = x + jnp.where(sub < 1, 0.0 if last1 is None else last1, r)
                last1 = r
                r = pltpu.roll(x, 2, 0)
                x = x + jnp.where(sub < 2, 0.0 if last2 is None else last2, r)
                last2 = r
                r = pltpu.roll(x, 4, 0)
                x = x + jnp.where(sub < 4, 0.0 if last4 is None else last4, r)
                last4 = r
                x16 = x if last8 is None else x + last8
                last8 = x
                x32 = x16 if len(last16) < 2 else x16 + last16[-2]
                last16 = last16[-1:] + [x16]
                x64 = x32 if len(last32) < 4 else x32 + last32[-4]
                last32 = last32[-3:] + [x32]
                if SKIP_GROUPS <= g < own_groups:
                    x64 = x64 * inverse[rows_of(g), lanes]
                    sums[0, f, g - SKIP_GROUPS] += folded(x64)
                    sums[1, f, g - SKIP_GROUPS] += folded(x64 * x64)
                buf[f, rows_of(g), lanes] = x64
            return carry

        lax.fori_loop(0, fields, one_field, 0)
        return carry

    lax.fori_loop(0, assets // width, chunk, 0)
    lane = lanes_iota()
    tiles = [jnp.zeros((GROUP, LANE), jnp.float32) for _ in range(2)]
    for stat in range(2):
        for f in range(fields):
            for g in range(main):
                tiles[stat] = jnp.where(lane == f * main + g, total_of(sums[stat, f, g]), tiles[stat])
    first = fields * main
    for g in range(main):
        tiles[0] = jnp.where(lane == first + g, total_of(counts[LATE_GROUPS + g]), tiles[0])
    for side in range(2):
        for g in range(LATE_GROUPS):
            spot = lane - (first + side * fields * LATE_GROUPS)
            here = (spot >= 0) & (spot < fields * LATE_GROUPS) & (lax.rem(spot, LATE_GROUPS) == g)
            at = g if side == 0 else LATE_GROUPS + main + g
            tiles[1] = jnp.where(here, total_of(counts[at]), tiles[1])
    for d in range(pay.shape[0]):
        pay[d, :GROUP, :] = tiles[0]
        pay[d, GROUP:, :] = tiles[1]


def row_moments(source, mine, inverse, where, cs, ss):
    fields, _, assets = source.shape
    width = 2 * LANE
    acc = [None] * (2 * fields)

    def added(i, x):
        acc[i] = x if acc[i] is None else acc[i] + x

    for at in range(0, assets, width):
        lanes = pl.ds(at, width)
        listed = inverse[where, lanes] > 0.0
        for f in range(fields):
            z = clipped_score(source[f, mine, lanes], cs[f], ss[f])
            z = jnp.where(listed, z, 0.0)
            added(f, folded(z))
            added(fields + f, folded(z * z))
    return acc


def second_pass(gathered, buf, inverse, stats, part):
    fields, _, assets = buf.shape
    main = (inverse.shape[0] - LATE) // GROUP - SKIP_GROUPS
    first = fields * main
    total = summed(gathered)
    t0, t1 = total[:GROUP], total[GROUP:]
    lane = lanes_iota()
    present = t1
    for f in range(fields):
        moved = pltpu.roll(t0, (f * main - first) % LANE, 1)
        present = jnp.where((lane >= f * main) & (lane < (f + 1) * main), moved, present)
    present = jnp.maximum(present, 1.0)
    center, scale = moments(t0, t1, present)
    stats[0], stats[1], stats[2] = center, scale, present
    width = 2 * LANE
    tiles = [jnp.zeros((GROUP, LANE), jnp.float32) for _ in range(2)]
    for g in range(main):
        rows = rows_of(g + SKIP_GROUPS)
        cs = [column(center, f * main + g, width) for f in range(fields)]
        ss = [column(scale, f * main + g, width) for f in range(fields)]

        acc = row_moments(buf, rows, inverse, rows, cs, ss)
        for f in range(fields):
            for stat in range(2):
                tiles[stat] = jnp.where(
                    lane == f * main + g, total_of(acc[stat * fields + f]), tiles[stat]
                )
    part[:GROUP, :] = tiles[0]
    part[GROUP:, :] = tiles[1]


def late_first_pass(buf, tail, head, from_ref, inverse, part, late, whole, pay):
    fields, _, assets = buf.shape
    rows = inverse.shape[0] - LATE
    base, base_next = block_starts(rows)
    follows = jnp.where(base_next > 0, 1.0, 0.0)
    width = 4 * LANE
    sub = sublanes(width)
    lane = lanes_iota()
    first = LANE - 2 * fields * LATE_GROUPS
    tiles = [part[:GROUP, :], part[GROUP:, :]]
    for f in range(fields):

        def tile(i, acc):
            lanes = pl.ds(pl.multiple_of(i * width, width), width)
            age = sub - jnp.maximum(from_ref[:, lanes], 0)
            acc = list(acc)
            for side, ref, at in ((0, tail, base - LATE), (1, head, base_next)):
                start = age + at
                masked = [
                    jnp.where(start >= -g * GROUP, ref[f, rows_of(g), lanes], 0.0)
                    for g in range(LATE_GROUPS)
                ]
                running, last = prefix_groups(masked, width)
                if side == 0:
                    whole[f, :, lanes] = last
                for g in range(LATE_GROUPS):
                    if side == 0:
                        where = rows_of(LATE_GROUPS + g)
                        r = buf[f, where, lanes] + (last - running[g])
                    else:
                        where = rows_of(rows // GROUP + g)
                        r = buf[f, where, lanes] * follows + running[g]
                    r = r * inverse[where, lanes]
                    late[f, rows_of(side * LATE_GROUPS + g), lanes] = r
                    k = side * LATE_GROUPS + g
                    acc[k] = acc[k] + folded(r)
                    acc[2 * LATE_GROUPS + k] = acc[2 * LATE_GROUPS + k] + folded(r * r)
            return tuple(acc)

        zero = jnp.zeros((GROUP, LANE), jnp.float32)
        acc = lax.fori_loop(0, assets // width, tile, (zero,) * (4 * LATE_GROUPS))
        for side in range(2):
            for g in range(LATE_GROUPS):
                spot = first + (side * fields + f) * LATE_GROUPS + g
                for stat in range(2):
                    value = total_of(acc[(stat * 2 + side) * LATE_GROUPS + g])
                    tiles[stat] = jnp.where(lane == spot, value, tiles[stat])
    for d in range(pay.shape[0]):
        pay[d, :GROUP, :] = tiles[0]
        pay[d, GROUP:, :] = tiles[1]


def late_second_pass(gathered, stats, late, inverse, level, pay):
    fields, _, assets = late.shape
    rows = inverse.shape[0] - LATE
    total = summed(gathered)
    center, scale = moments(total[:GROUP], total[GROUP:], stats[2])
    level[0], level[1] = center, scale
    width = 2 * LANE
    first = LANE - 2 * fields * LATE_GROUPS
    lane = lanes_iota()
    out = jnp.zeros((GROUP, LANE), jnp.float32)
    for side in range(2):
        for g in range(LATE_GROUPS):
            spots = [first + (side * fields + f) * LATE_GROUPS + g for f in range(fields)]
            cs = [column(center, spot, width) for spot in spots]
            ss = [column(scale, spot, width) for spot in spots]
            where = rows_of(LATE_GROUPS + g if side == 0 else rows // GROUP + g)
            mine = rows_of(side * LATE_GROUPS + g)

            acc = row_moments(late, mine, inverse, where, cs, ss)
            back = LANE - first
            for f in range(fields):
                out = jnp.where(lane == spots[f], total_of(acc[f]), out)
                out = jnp.where(lane == spots[f] - back, total_of(acc[fields + f]), out)
    for d in range(pay.shape[0]):
        pay[d] = out


def final_rows(f, where, source, mine, inverse, stage, put, cols, assets):
    width = 2 * LANE
    c1, s1, c2, s2 = cols
    for at in range(0, assets, width):
        lanes = pl.ds(at, width)
        z = clipped_score(source[f, mine, lanes], c1, s1)
        z = (z - c2) * s2
        stage[f, put, lanes] = jnp.where(inverse[where, lanes] > 0.0, z, 0.0)


def main_final_pass(buf, inverse, stats, level, out, stage, sems):
    fields, rows, assets = out.shape
    main = rows // GROUP - SKIP_GROUPS
    width = 2 * LANE
    c1, s1, c2, s2 = stats[0], stats[1], level[0], level[1]
    copies = []
    for f in range(fields):
        for g in range(main):
            spot = f * main + g
            where = rows_of(g + SKIP_GROUPS)
            cols = [column(t, spot, width) for t in (c1, s1, c2, s2)]
            final_rows(f, where, buf, where, inverse, stage, rows_of(g), cols, assets)
        copy = pltpu.make_async_copy(
            stage.at[f], out.at[f, pl.ds(WINDOW, rows - WINDOW), :], sems.at[f]
        )
        copy.start()
        copies.append(copy)
    for copy in copies:
        copy.wait()


def send_pass(gathered, stats, level, level4, pay):
    total = summed(gathered)
    back = 32
    square = pltpu.roll(total, back, 1)
    center, scale = moments(total, square, stats[2])
    level4[0], level4[1] = center, scale
    lane = lanes_iota()
    out = jnp.zeros((GROUP, LANE), jnp.float32)
    for i, t in enumerate((level[0], level[1], center, scale)):
        moved = pltpu.roll(t, 16 * (i + 1), 1)
        out = jnp.where((lane >= 16 * i) & (lane < 16 * (i + 1)), moved, out)
    pay[...] = out


def late_final_pass(late, inverse, level, level4, prior, out, stage, sems):
    fields, _, assets = late.shape
    width = 2 * LANE
    first = LANE - 2 * fields * LATE_GROUPS
    copies = []
    for f in range(fields):
        for g in range(LATE_GROUPS):
            spot = first + f * LATE_GROUPS + g
            tiles = (level[0], level[1], level4[0], level4[1])
            cols = [column(t, spot, width) for t in tiles]
            where = rows_of(LATE_GROUPS + g)
            final_rows(f, where, late, rows_of(g), inverse, stage, rows_of(g), cols, assets)
        copy = pltpu.make_async_copy(stage.at[f], out.at[f, pl.ds(LATE, LATE), :], sems.at[f])
        copy.start()
        copies.append(copy)
    for copy in copies:
        copy.wait()


def head_final_pass(buf, tail, whole, from_ref, inverse, sent, prior, out, stage, sems):
    fields, _, assets = buf.shape
    base = block_starts(inverse.shape[0] - LATE)[0]
    width = 4 * LANE
    sub = sublanes(width)
    levels = sent[...]
    copies = []
    for f in range(fields):
        cols = [
            [column(levels, 16 * i + f * LATE_GROUPS + g, width) for i in range(4)]
            for g in range(LATE_GROUPS)
        ]

        def tile(i, carry):
            lanes = pl.ds(pl.multiple_of(i * width, width), width)
            start = sub - jnp.maximum(from_ref[:, lanes], 0) + (base - WINDOW)
            masked = [
                jnp.where(start >= -g * GROUP, tail[f, rows_of(g), lanes], 0.0)
                for g in range(LATE_GROUPS)
            ]
            running, last = prefix_groups(masked, width)
            last = last + whole[f, :, lanes]
            for g in range(LATE_GROUPS):
                c1, s1, c2, s2 = cols[g]
                weight = inverse[rows_of(g), lanes]
                r = (buf[f, rows_of(g), lanes] + (last - running[g])) * weight
                z = (clipped_score(r, c1, s1) - c2) * s2
                stage[f, rows_of(g), lanes] = jnp.where(weight > 0.0, z, 0.0)
            return carry

        lax.fori_loop(0, assets // width, tile, 0)
        copy = pltpu.make_async_copy(stage.at[f], out.at[f, pl.ds(0, LATE), :], sems.at[f])
        copy.start()
        copies.append(copy)
    for copy in copies:
        copy.wait()


def shape(*dims):
    return jax.ShapeDtypeStruct(dims, jnp.float32)


def call(body, name, ins, outs, out_specs, scratch=(), limit=8, flops=0, aliases=None):
    return pl.pallas_call(
        body,
        name=name,
        out_shape=outs,
        in_specs=ins,
        out_specs=out_specs,
        scratch_shapes=list(scratch),
        input_output_aliases=aliases or {},
        compiler_params=pltpu.CompilerParams(vmem_limit_bytes=limit * MIB),
        cost_estimate=pl.CostEstimate(flops=flops, bytes_accessed=0, transcendentals=0),
    )


def per_device(values, listed_from, listed_until):
    fields, rows, assets = values.shape
    n = lax.axis_size("asset")
    blocks = lax.axis_size("tm")
    forward = [(i, i + 1) for i in range(blocks - 1)]
    ring = [(i, (i + 1) % blocks) for i in range(blocks)]
    back = [((i + 1) % blocks, i) for i in range(blocks)]
    work = fields * rows * assets
    slab = shape(fields, LATE, assets)
    near, head, held = call(
        load, "load", [HBM], (slab, slab, shape(fields, rows, assets)), (VMEM,) * 3,
        [pltpu.SemaphoreType.DMA((3,))], limit=40, flops=work // 8,
    )(values)
    tail_near = lax.ppermute(near, "tm", forward)
    head = lax.ppermute(head, "tm", back)
    opened, closed = listed_from.reshape(1, assets), listed_until.reshape(1, assets)
    main = rows // GROUP - SKIP_GROUPS
    tile = shape(GROUP, LANE)
    pair = shape(2, GROUP, LANE)
    exchange = functools.partial(
        lax.all_to_all, axis_name="asset", split_axis=0, concat_axis=0, tiled=True
    )

    buf, inverse, pay, far = call(
        first_pass, "first_pass", [VMEM, HBM, HBM],
        (
            shape(fields, rows + LATE, assets), shape(rows + LATE, assets),
            shape(n, 2 * GROUP, LANE), slab,
        ),
        (VMEM,) * 4,
        [
            pltpu.VMEM((1, assets), jnp.int32),
            pltpu.VMEM((1, assets), jnp.int32),
            pltpu.VMEM((2, fields, main, GROUP, LANE), jnp.float32),
            pltpu.VMEM((main + 2 * LATE_GROUPS, GROUP, LANE), jnp.float32),
            pltpu.SemaphoreType.DMA((2,)),
        ],
        limit=8, flops=20 * work,
    )(held, opened, closed)
    tail_far = lax.ppermute(far, "tm", forward)
    gathered = exchange(pay)
    stats, part = call(
        second_pass, "second_pass", [VMEM] * 3,
        (shape(3, GROUP, LANE), shape(2 * GROUP, LANE)), (VMEM, VMEM), limit=16, flops=10 * work,
    )(gathered, buf, inverse)
    late, whole, pay = call(
        late_first_pass, "late_first_pass", [VMEM] * 6,
        (shape(fields, 2 * LATE, assets), shape(fields, GROUP, assets), shape(n, 2 * GROUP, LANE)),
        (VMEM, VMEM, VMEM), limit=20, flops=5 * work,
    )(buf, tail_near, head, opened, inverse, part)
    gathered = exchange(pay)
    level, pay = call(
        late_second_pass, "late_second_pass", [VMEM] * 4,
        (pair, shape(n, GROUP, LANE)), (VMEM, VMEM), limit=16, flops=3 * work,
    )(gathered, stats, late, inverse)
    gathered = exchange(pay)
    out = call(
        main_final_pass, "main_final_pass", [VMEM] * 4,
        shape(fields, rows, assets), HBM,
        [
            pltpu.VMEM((fields, rows - WINDOW, assets), jnp.float32),
            pltpu.SemaphoreType.DMA((fields,)),
        ],
        limit=20, flops=10 * work,
    )(buf, inverse, stats, level)
    level4, pay = call(
        send_pass, "send_pass", [VMEM] * 3, (pair, tile), (VMEM, VMEM), flops=work // 100,
    )(gathered, stats, level)
    sent = lax.ppermute(pay, "tm", ring)
    stage = [
        pltpu.VMEM((fields, LATE, assets), jnp.float32),
        pltpu.SemaphoreType.DMA((fields,)),
    ]
    out = call(
        late_final_pass, "late_final_pass", [VMEM] * 4 + [HBM],
        shape(fields, rows, assets), HBM, stage, limit=16, flops=2 * work, aliases={4: 0},
    )(late, inverse, level, level4, out)
    return call(
        head_final_pass, "head_final_pass", [VMEM] * 6 + [HBM],
        shape(fields, rows, assets), HBM, stage, limit=16, flops=2 * work, aliases={6: 0},
    )(buf, tail_far, whole, opened, inverse, sent, out)


def solution(mesh):
    in_specs = (P(None, "tm", "asset"), P("asset"), P("asset"))
    out_specs = P(None, "tm", "asset")
    return jax.shard_map(
        per_device, mesh=mesh, in_specs=in_specs, out_specs=out_specs, check_vma=False
    )
```

```python
import functools

import jax
import jax.numpy as jnp
from jax import lax
from jax.experimental import pallas as pl
from jax.experimental.pallas import tpu as pltpu
from jax.sharding import PartitionSpec as P

WINDOW = 64
EPS = 0.1
LIMIT = 3.0
GROUP = 8
LANE = 128
LATE = 32
LATE_GROUPS = LATE // GROUP
SKIP_GROUPS = WINDOW // GROUP
VMEM = pl.BlockSpec(memory_space=pltpu.VMEM)
HBM = pl.BlockSpec(memory_space=pltpu.HBM)
MIB = 1 << 20


def rows_of(g):
    return pl.ds(g * GROUP, GROUP)


def block_starts(rows):
    block, blocks = lax.axis_index("tm"), lax.axis_size("tm")
    return block * rows, lax.rem(block + 1, blocks) * rows


def sublanes(width):
    return lax.broadcasted_iota(jnp.int32, (GROUP, width), 0)


def lanes_iota():
    return lax.broadcasted_iota(jnp.int32, (GROUP, LANE), 1)


def folded(x):
    total = x[:, :LANE]
    for at in range(LANE, x.shape[1], LANE):
        total = total + x[:, at : at + LANE]
    return total


def total_of(x):
    return jnp.sum(x, axis=1, keepdims=True)


def column(tile, lane, width):
    return jnp.broadcast_to(tile[:, lane : lane + 1], (GROUP, width))


def clipped_score(x, center, scale):
    return jnp.minimum(jnp.maximum((x - center) * scale, -LIMIT), LIMIT)


def moments(total, square, present):
    center = total / present
    spread = jnp.maximum(square / present - center * center, 0.0)
    return center, 1.0 / jnp.sqrt(spread + EPS)


def summed(gathered):
    total = gathered[0]
    for d in range(1, gathered.shape[0]):
        total = total + gathered[d]
    return total


def prefix_groups(groups, width):
    sub = sublanes(width)
    carried, out = None, []
    for x in groups:
        for s in (1, 2, 4):
            x = x + jnp.where(sub < s, 0.0, pltpu.roll(x, s, 0))
        if carried is not None:
            x = x + carried
        carried = jnp.broadcast_to(x[GROUP - 1 :, :], (GROUP, width))
        out.append(x)
    return out, carried


def cut(x_hbm, near, head, sems):
    rows = x_hbm.shape[1]
    copies = [
        pltpu.make_async_copy(x_hbm.at[:, pl.ds(rows - LATE, LATE), :], near, sems.at[0]),
        pltpu.make_async_copy(x_hbm.at[:, pl.ds(0, LATE), :], head, sems.at[1]),
    ]
    for copy in copies:
        copy.start()
    for copy in copies:
        copy.wait()


def load(x_hbm, from_hbm, until_hbm, x_ref, inverse, tally, from_ref, until_ref, sems):
    fields, rows, assets = x_hbm.shape
    own_groups = rows // GROUP
    groups = own_groups + LATE_GROUPS
    main = own_groups - SKIP_GROUPS
    base, base_next = block_starts(rows)
    dates = [
        pltpu.make_async_copy(from_hbm, from_ref, sems.at[0]),
        pltpu.make_async_copy(until_hbm, until_ref, sems.at[1]),
    ]
    whole = pltpu.make_async_copy(x_hbm, x_ref, sems.at[2])
    for copy in dates:
        copy.start()
    whole.start()
    width = 4 * LANE
    sub = sublanes(width)
    for copy in dates:
        copy.wait()
    lane = lanes_iota()
    first = fields * main
    tiles = [jnp.zeros((GROUP, LANE), jnp.float32) for _ in range(2)]
    for g in range(groups):
        at = base + g * GROUP if g < own_groups else base_next + (g - own_groups) * GROUP
        count = jnp.zeros((GROUP, LANE), jnp.float32)
        for start in range(0, assets, width):
            lanes = pl.ds(start, width)
            seen = sub - jnp.maximum(from_ref[:, lanes], 0) + at
            listed = (seen >= 0) & (until_ref[:, lanes] - sub > at)
            counted = jnp.clip(seen + 1, 1, WINDOW).astype(jnp.float32)
            inverse[rows_of(g), lanes] = jnp.where(listed, 1.0 / counted, 0.0)
            count = count + folded(jnp.where(listed, 1.0, 0.0))
        if SKIP_GROUPS <= g < own_groups:
            tiles[0] = jnp.where(lane == first + g - SKIP_GROUPS, total_of(count), tiles[0])
        elif g >= SKIP_GROUPS - LATE_GROUPS:
            side = 0 if g < SKIP_GROUPS else 1
            k = g - LATE_GROUPS if side == 0 else g - own_groups
            spot = lane - (first + side * fields * LATE_GROUPS)
            here = (spot >= 0) & (spot < fields * LATE_GROUPS) & (lax.rem(spot, LATE_GROUPS) == k)
            tiles[1] = jnp.where(here, total_of(count), tiles[1])
    tally[:GROUP, :] = tiles[0]
    tally[GROUP:, :] = tiles[1]
    whole.wait()


def first_pass(x_ref, from_ref, inverse, tally, buf, pay, far, sums):
    fields, rows, assets = x_ref.shape
    own_groups = rows // GROUP
    groups = own_groups + LATE_GROUPS
    main = own_groups - SKIP_GROUPS
    width = 2 * LANE
    base = block_starts(rows)[0]
    sums[...] = jnp.zeros_like(sums)
    sub = sublanes(width)

    def chunk(c, carry):
        lanes = pl.ds(pl.multiple_of(c * width, width), width)
        start = base + sub - jnp.maximum(from_ref[:, lanes], 0)

        def one_field(f, carry):
            last1 = last2 = last4 = last8 = None
            last16, last32 = [], []
            for g in range(groups):
                if own_groups - SKIP_GROUPS <= g < own_groups - LATE_GROUPS:
                    to = rows_of(g - (own_groups - SKIP_GROUPS))
                    far[f, to, lanes] = x_ref[f, rows_of(g), lanes]
                if g < own_groups:
                    x = jnp.where(start >= -g * GROUP, x_ref[f, rows_of(g), lanes], 0.0)
                else:
                    x = jnp.zeros((GROUP, width), jnp.float32)
                r = pltpu.roll(x, 1, 0)
                x = x + jnp.where(sub < 1, 0.0 if last1 is None else last1, r)
                last1 = r
                r = pltpu.roll(x, 2, 0)
                x = x + jnp.where(sub < 2, 0.0 if last2 is None else last2, r)
                last2 = r
                r = pltpu.roll(x, 4, 0)
                x = x + jnp.where(sub < 4, 0.0 if last4 is None else last4, r)
                last4 = r
                x16 = x if last8 is None else x + last8
                last8 = x
                x32 = x16 if len(last16) < 2 else x16 + last16[-2]
                last16 = last16[-1:] + [x16]
                x64 = x32 if len(last32) < 4 else x32 + last32[-4]
                last32 = last32[-3:] + [x32]
                if SKIP_GROUPS <= g < own_groups:
                    x64 = x64 * inverse[rows_of(g), lanes]
                    sums[0, f, g - SKIP_GROUPS] += folded(x64)
                    sums[1, f, g - SKIP_GROUPS] += folded(x64 * x64)
                buf[f, rows_of(g), lanes] = x64
            return carry

        lax.fori_loop(0, fields, one_field, 0)
        return carry

    lax.fori_loop(0, assets // width, chunk, 0)
    lane = lanes_iota()
    tiles = [tally[:GROUP, :], tally[GROUP:, :]]
    for stat in range(2):
        for f in range(fields):
            for g in range(main):
                tiles[stat] = jnp.where(lane == f * main + g, total_of(sums[stat, f, g]), tiles[stat])
    for d in range(pay.shape[0]):
        pay[d, :GROUP, :] = tiles[0]
        pay[d, GROUP:, :] = tiles[1]


def row_moments(source, mine, inverse, where, cs, ss):
    fields, _, assets = source.shape
    width = 2 * LANE
    acc = [None] * (2 * fields)

    def added(i, x):
        acc[i] = x if acc[i] is None else acc[i] + x

    for at in range(0, assets, width):
        lanes = pl.ds(at, width)
        listed = inverse[where, lanes] > 0.0
        for f in range(fields):
            z = clipped_score(source[f, mine, lanes], cs[f], ss[f])
            z = jnp.where(listed, z, 0.0)
            added(f, folded(z))
            added(fields + f, folded(z * z))
    return acc


def second_pass(gathered, buf, inverse, stats, part):
    fields, _, assets = buf.shape
    main = (inverse.shape[0] - LATE) // GROUP - SKIP_GROUPS
    first = fields * main
    total = summed(gathered)
    t0, t1 = total[:GROUP], total[GROUP:]
    lane = lanes_iota()
    present = t1
    for f in range(fields):
        moved = pltpu.roll(t0, (f * main - first) % LANE, 1)
        present = jnp.where((lane >= f * main) & (lane < (f + 1) * main), moved, present)
    present = jnp.maximum(present, 1.0)
    center, scale = moments(t0, t1, present)
    stats[0], stats[1], stats[2] = center, scale, present
    width = 2 * LANE
    tiles = [jnp.zeros((GROUP, LANE), jnp.float32) for _ in range(2)]
    for g in range(main):
        rows = rows_of(g + SKIP_GROUPS)
        cs = [column(center, f * main + g, width) for f in range(fields)]
        ss = [column(scale, f * main + g, width) for f in range(fields)]

        acc = row_moments(buf, rows, inverse, rows, cs, ss)
        for f in range(fields):
            for stat in range(2):
                tiles[stat] = jnp.where(
                    lane == f * main + g, total_of(acc[stat * fields + f]), tiles[stat]
                )
    part[:GROUP, :] = tiles[0]
    part[GROUP:, :] = tiles[1]


def late_first_pass(buf, tail, head, from_ref, inverse, part, late, whole, pay):
    fields, _, assets = buf.shape
    rows = inverse.shape[0] - LATE
    base, base_next = block_starts(rows)
    follows = jnp.where(base_next > 0, 1.0, 0.0)
    width = 4 * LANE
    sub = sublanes(width)
    lane = lanes_iota()
    first = LANE - 2 * fields * LATE_GROUPS
    tiles = [part[:GROUP, :], part[GROUP:, :]]
    for f in range(fields):

        def tile(i, acc):
            lanes = pl.ds(pl.multiple_of(i * width, width), width)
            age = sub - jnp.maximum(from_ref[:, lanes], 0)
            acc = list(acc)
            for side, ref, at in ((0, tail, base - LATE), (1, head, base_next)):
                start = age + at
                masked = [
                    jnp.where(start >= -g * GROUP, ref[f, rows_of(g), lanes], 0.0)
                    for g in range(LATE_GROUPS)
                ]
                running, last = prefix_groups(masked, width)
                if side == 0:
                    whole[f, :, lanes] = last
                for g in range(LATE_GROUPS):
                    if side == 0:
                        where = rows_of(LATE_GROUPS + g)
                        r = buf[f, where, lanes] + (last - running[g])
                    else:
                        where = rows_of(rows // GROUP + g)
                        r = buf[f, where, lanes] * follows + running[g]
                    r = r * inverse[where, lanes]
                    late[f, rows_of(side * LATE_GROUPS + g), lanes] = r
                    k = side * LATE_GROUPS + g
                    acc[k] = acc[k] + folded(r)
                    acc[2 * LATE_GROUPS + k] = acc[2 * LATE_GROUPS + k] + folded(r * r)
            return tuple(acc)

        zero = jnp.zeros((GROUP, LANE), jnp.float32)
        acc = lax.fori_loop(0, assets // width, tile, (zero,) * (4 * LATE_GROUPS))
        for side in range(2):
            for g in range(LATE_GROUPS):
                spot = first + (side * fields + f) * LATE_GROUPS + g
                for stat in range(2):
                    value = total_of(acc[(stat * 2 + side) * LATE_GROUPS + g])
                    tiles[stat] = jnp.where(lane == spot, value, tiles[stat])
    for d in range(pay.shape[0]):
        pay[d, :GROUP, :] = tiles[0]
        pay[d, GROUP:, :] = tiles[1]


def late_second_pass(gathered, stats, late, inverse, level, pay):
    fields, _, assets = late.shape
    rows = inverse.shape[0] - LATE
    total = summed(gathered)
    center, scale = moments(total[:GROUP], total[GROUP:], stats[2])
    level[0], level[1] = center, scale
    width = 2 * LANE
    first = LANE - 2 * fields * LATE_GROUPS
    lane = lanes_iota()
    out = jnp.zeros((GROUP, LANE), jnp.float32)
    for side in range(2):
        for g in range(LATE_GROUPS):
            spots = [first + (side * fields + f) * LATE_GROUPS + g for f in range(fields)]
            cs = [column(center, spot, width) for spot in spots]
            ss = [column(scale, spot, width) for spot in spots]
            where = rows_of(LATE_GROUPS + g if side == 0 else rows // GROUP + g)
            mine = rows_of(side * LATE_GROUPS + g)

            acc = row_moments(late, mine, inverse, where, cs, ss)
            back = LANE - first
            for f in range(fields):
                out = jnp.where(lane == spots[f], total_of(acc[f]), out)
                out = jnp.where(lane == spots[f] - back, total_of(acc[fields + f]), out)
    for d in range(pay.shape[0]):
        pay[d] = out


def final_rows(f, where, source, mine, inverse, stage, put, cols, assets):
    width = 2 * LANE
    c1, s1, c2, s2 = cols
    for at in range(0, assets, width):
        lanes = pl.ds(at, width)
        z = clipped_score(source[f, mine, lanes], c1, s1)
        z = (z - c2) * s2
        stage[f, put, lanes] = jnp.where(inverse[where, lanes] > 0.0, z, 0.0)


def send_pass(gathered, stats, level, level4, pay):
    total = summed(gathered)
    back = 32
    square = pltpu.roll(total, back, 1)
    center, scale = moments(total, square, stats[2])
    level4[0], level4[1] = center, scale
    lane = lanes_iota()
    out = jnp.zeros((GROUP, LANE), jnp.float32)
    for i, t in enumerate((level[0], level[1], center, scale)):
        moved = pltpu.roll(t, 16 * (i + 1), 1)
        out = jnp.where((lane >= 16 * i) & (lane < 16 * (i + 1)), moved, out)
    pay[...] = out


def final_pass(
    buf, late, tail, whole, from_ref, inverse, stats, level, level4,
    out, rolled, stage, sems,
):
    fields, rows, assets = out.shape
    main = rows // GROUP - SKIP_GROUPS
    first = LANE - 2 * fields * LATE_GROUPS
    width = 2 * LANE
    late_tiles = (level[0], level[1], level4[0], level4[1])
    main_tiles = (stats[0], stats[1], level[0], level[1])
    copies = []
    for f in range(fields):
        for g in range(LATE_GROUPS):
            spot = first + f * LATE_GROUPS + g
            cols = [column(t, spot, width) for t in late_tiles]
            where = rows_of(LATE_GROUPS + g)
            final_rows(f, where, late, rows_of(g), inverse, stage, rows_of(g), cols, assets)
        for g in range(main):
            cols = [column(t, f * main + g, width) for t in main_tiles]
            where = rows_of(g + SKIP_GROUPS)
            put = rows_of(LATE_GROUPS + g)
            final_rows(f, where, buf, where, inverse, stage, put, cols, assets)
        copy = pltpu.make_async_copy(
            stage.at[f], out.at[f, pl.ds(LATE, rows - LATE), :], sems.at[f]
        )
        copy.start()
        copies.append(copy)
    base = block_starts(rows)[0]
    width = 4 * LANE
    sub = sublanes(width)
    for f in range(fields):

        def tile(i, carry):
            lanes = pl.ds(pl.multiple_of(i * width, width), width)
            start = sub - jnp.maximum(from_ref[:, lanes], 0) + (base - WINDOW)
            masked = [
                jnp.where(start >= -g * GROUP, tail[f, rows_of(g), lanes], 0.0)
                for g in range(LATE_GROUPS)
            ]
            running, last = prefix_groups(masked, width)
            last = last + whole[f, :, lanes]
            for g in range(LATE_GROUPS):
                r = buf[f, rows_of(g), lanes] + (last - running[g])
                rolled[f, rows_of(g), lanes] = r * inverse[rows_of(g), lanes]
            return carry

        lax.fori_loop(0, assets // width, tile, 0)
    for copy in copies:
        copy.wait()


def head_final_pass(rolled, inverse, sent, prior, out, stage, sems):
    fields, _, assets = rolled.shape
    width = 2 * LANE
    levels = sent[...]
    copies = []
    for f in range(fields):
        for g in range(LATE_GROUPS):
            cols = [column(levels, 16 * i + f * LATE_GROUPS + g, width) for i in range(4)]
            rows = rows_of(g)
            final_rows(f, rows, rolled, rows, inverse, stage, rows, cols, assets)
        copy = pltpu.make_async_copy(stage.at[f], out.at[f, pl.ds(0, LATE), :], sems.at[f])
        copy.start()
        copies.append(copy)
    for copy in copies:
        copy.wait()


def shape(*dims):
    return jax.ShapeDtypeStruct(dims, jnp.float32)


def call(body, name, ins, outs, out_specs, scratch=(), limit=8, flops=0, aliases=None):
    return pl.pallas_call(
        body,
        name=name,
        out_shape=outs,
        in_specs=ins,
        out_specs=out_specs,
        scratch_shapes=list(scratch),
        input_output_aliases=aliases or {},
        compiler_params=pltpu.CompilerParams(vmem_limit_bytes=limit * MIB),
        cost_estimate=pl.CostEstimate(flops=flops, bytes_accessed=0, transcendentals=0),
    )


def per_device(values, listed_from, listed_until):
    fields, rows, assets = values.shape
    n = lax.axis_size("asset")
    blocks = lax.axis_size("tm")
    ring = [(i, (i + 1) % blocks) for i in range(blocks)]
    back = [((i + 1) % blocks, i) for i in range(blocks)]
    work = fields * rows * assets
    slab = shape(fields, LATE, assets)
    near, head = call(
        cut, "cut", [HBM], (slab, slab), (VMEM, VMEM), [pltpu.SemaphoreType.DMA((2,))],
        limit=50,
    )(values)
    tail_near = lax.ppermute(near, "tm", ring)
    head = lax.ppermute(head, "tm", back)
    opened, closed = listed_from.reshape(1, assets), listed_until.reshape(1, assets)
    main = rows // GROUP - SKIP_GROUPS
    tile = shape(GROUP, LANE)
    pair = shape(2, GROUP, LANE)
    exchange = functools.partial(
        lax.all_to_all, axis_name="asset", split_axis=0, concat_axis=0, tiled=True
    )

    held, inverse, tally = call(
        load, "load", [HBM] * 3,
        (shape(fields, rows, assets), shape(rows + LATE, assets), shape(2 * GROUP, LANE)),
        (VMEM,) * 3,
        [
            pltpu.VMEM((1, assets), jnp.int32),
            pltpu.VMEM((1, assets), jnp.int32),
            pltpu.SemaphoreType.DMA((3,)),
        ],
        limit=40, flops=work,
    )(values, opened, closed)
    buf, pay, far = call(
        first_pass, "first_pass", [VMEM] * 4,
        (shape(fields, rows + LATE, assets), shape(n, 2 * GROUP, LANE), slab),
        (VMEM,) * 3,
        [pltpu.VMEM((2, fields, main, GROUP, LANE), jnp.float32)], flops=20 * work,
    )(held, opened, inverse, tally)
    tail_far = lax.ppermute(far, "tm", ring)
    gathered = exchange(pay)
    stats, part = call(
        second_pass, "second_pass", [VMEM] * 3,
        (shape(3, GROUP, LANE), shape(2 * GROUP, LANE)), (VMEM, VMEM), limit=16, flops=10 * work,
    )(gathered, buf, inverse)
    late, whole, pay = call(
        late_first_pass, "late_first_pass", [VMEM] * 6,
        (shape(fields, 2 * LATE, assets), shape(fields, GROUP, assets), shape(n, 2 * GROUP, LANE)),
        (VMEM, VMEM, VMEM), limit=20, flops=5 * work,
    )(buf, tail_near, head, opened, inverse, part)
    gathered = exchange(pay)
    level, pay = call(
        late_second_pass, "late_second_pass", [VMEM] * 4,
        (pair, shape(n, GROUP, LANE)), (VMEM, VMEM), limit=16, flops=3 * work,
    )(gathered, stats, late, inverse)
    gathered = exchange(pay)
    level4, pay = call(
        send_pass, "send_pass", [VMEM] * 3, (pair, tile), (VMEM, VMEM), flops=work // 100,
    )(gathered, stats, level)
    sent = lax.ppermute(pay, "tm", ring)
    out, rolled = call(
        final_pass, "final_pass", [VMEM] * 9,
        (shape(fields, rows, assets), slab), (HBM, VMEM),
        [
            pltpu.VMEM((fields, rows - LATE, assets), jnp.float32),
            pltpu.SemaphoreType.DMA((fields,)),
        ],
        limit=16, flops=10 * work,
    )(buf, late, tail_far, whole, opened, inverse, stats, level, level4)
    return call(
        head_final_pass, "head_final_pass", [VMEM] * 3 + [HBM],
        shape(fields, rows, assets), HBM,
        [pltpu.VMEM((fields, LATE, assets), jnp.float32), pltpu.SemaphoreType.DMA((fields,))],
        limit=16, flops=2 * work, aliases={3: 0},
    )(rolled, inverse, sent, out)


def solution(mesh):
    in_specs = (P(None, "tm", "asset"), P("asset"), P("asset"))
    out_specs = P(None, "tm", "asset")
    return jax.shard_map(
        per_device, mesh=mesh, in_specs=in_specs, out_specs=out_specs, check_vma=False
    )
```

```python
import functools

import jax
import jax.numpy as jnp
from jax import lax
from jax.experimental import pallas as pl
from jax.experimental.pallas import tpu as pltpu
from jax.sharding import PartitionSpec as P

WINDOW = 64
EPS = 0.1
LIMIT = 3.0
GROUP = 8
LANE = 128
LATE = 32
LATE_GROUPS = LATE // GROUP
SKIP_GROUPS = WINDOW // GROUP
VMEM = pl.BlockSpec(memory_space=pltpu.VMEM)
HBM = pl.BlockSpec(memory_space=pltpu.HBM)
MIB = 1 << 20


def rows_of(g):
    return pl.ds(g * GROUP, GROUP)


def block_starts(rows):
    block, blocks = lax.axis_index("tm"), lax.axis_size("tm")
    return block * rows, lax.rem(block + 1, blocks) * rows


def sublanes(width):
    return lax.broadcasted_iota(jnp.int32, (GROUP, width), 0)


def lanes_iota():
    return lax.broadcasted_iota(jnp.int32, (GROUP, LANE), 1)


def folded(x):
    total = x[:, :LANE]
    for at in range(LANE, x.shape[1], LANE):
        total = total + x[:, at : at + LANE]
    return total


def total_of(x):
    return jnp.sum(x, axis=1, keepdims=True)


def column(tile, lane, width):
    return jnp.broadcast_to(tile[:, lane : lane + 1], (GROUP, width))


def clipped_score(x, center, scale):
    return jnp.minimum(jnp.maximum((x - center) * scale, -LIMIT), LIMIT)


def moments(total, square, present):
    center = total / present
    spread = jnp.maximum(square / present - center * center, 0.0)
    return center, 1.0 / jnp.sqrt(spread + EPS)


def summed(gathered):
    total = gathered[0]
    for d in range(1, gathered.shape[0]):
        total = total + gathered[d]
    return total


def prefix_groups(groups, width):
    sub = sublanes(width)
    carried, out = None, []
    for x in groups:
        for s in (1, 2, 4):
            x = x + jnp.where(sub < s, 0.0, pltpu.roll(x, s, 0))
        if carried is not None:
            x = x + carried
        carried = jnp.broadcast_to(x[GROUP - 1 :, :], (GROUP, width))
        out.append(x)
    return out, carried


def cut(x_hbm, near, head, sems):
    rows = x_hbm.shape[1]
    copies = [
        pltpu.make_async_copy(x_hbm.at[:, pl.ds(rows - LATE, LATE), :], near, sems.at[0]),
        pltpu.make_async_copy(x_hbm.at[:, pl.ds(0, LATE), :], head, sems.at[1]),
    ]
    for copy in copies:
        copy.start()
    for copy in copies:
        copy.wait()


def first_pass(
    x_hbm, from_hbm, until_hbm,
    edge, low, high, inverse, pay, far, from_ref, until_ref, xs, sums, sems, date_sems,
):
    fields, rows, assets = x_hbm.shape
    own_groups = rows // GROUP
    groups = own_groups + LATE_GROUPS
    main = own_groups - SKIP_GROUPS
    base, base_next = block_starts(rows)
    chunks, _, _, width = xs.shape

    def fetch(c):
        lanes = pl.ds(pl.multiple_of(c * width, width), width)
        return pltpu.make_async_copy(x_hbm.at[:, :, lanes], xs.at[c], sems.at[c])

    dates = [
        pltpu.make_async_copy(from_hbm, from_ref, date_sems.at[0]),
        pltpu.make_async_copy(until_hbm, until_ref, date_sems.at[1]),
    ]
    for copy in dates:
        copy.start()
    for c in range(chunks):
        fetch(c).start()
    sums[...] = jnp.zeros_like(sums)
    wide = 4 * LANE
    sub = sublanes(wide)
    lane = lanes_iota()
    first = fields * main
    tiles = [jnp.zeros((GROUP, LANE), jnp.float32) for _ in range(2)]
    for copy in dates:
        copy.wait()
    for g in range(groups):
        at = base + g * GROUP if g < own_groups else base_next + (g - own_groups) * GROUP
        count = jnp.zeros((GROUP, LANE), jnp.float32)
        for start in range(0, assets, wide):
            lanes = pl.ds(start, wide)
            seen = sub - jnp.maximum(from_ref[:, lanes], 0) + at
            listed = (seen >= 0) & (until_ref[:, lanes] - sub > at)
            counted = jnp.clip(seen + 1, 1, WINDOW).astype(jnp.float32)
            inverse[rows_of(g), lanes] = jnp.where(listed, 1.0 / counted, 0.0)
            count = count + folded(jnp.where(listed, 1.0, 0.0))
        if SKIP_GROUPS <= g < own_groups:
            tiles[0] = jnp.where(lane == first + g - SKIP_GROUPS, total_of(count), tiles[0])
        elif g >= SKIP_GROUPS - LATE_GROUPS:
            side = 0 if g < SKIP_GROUPS else 1
            k = g - LATE_GROUPS if side == 0 else g - own_groups
            spot = lane - (first + side * fields * LATE_GROUPS)
            here = (spot >= 0) & (spot < fields * LATE_GROUPS) & (lax.rem(spot, LATE_GROUPS) == k)
            tiles[1] = jnp.where(here, total_of(count), tiles[1])
    sub = sublanes(width)

    def chunk(c, carry):
        lanes = pl.ds(pl.multiple_of(c * width, width), width)
        start = base + sub - jnp.maximum(from_ref[:, lanes], 0)
        fetch(c).wait()

        def one_field(f, carry):
            last1 = last2 = last4 = last8 = None
            last16, last32 = [], []
            for g in range(groups):
                if own_groups - SKIP_GROUPS <= g < own_groups - LATE_GROUPS:
                    to = rows_of(g - (own_groups - SKIP_GROUPS))
                    far[f, to, lanes] = xs[c, f, rows_of(g), :]
                if g < own_groups:
                    x = jnp.where(start >= -g * GROUP, xs[c, f, rows_of(g), :], 0.0)
                else:
                    x = jnp.zeros((GROUP, width), jnp.float32)
                r = pltpu.roll(x, 1, 0)
                x = x + jnp.where(sub < 1, 0.0 if last1 is None else last1, r)
                last1 = r
                r = pltpu.roll(x, 2, 0)
                x = x + jnp.where(sub < 2, 0.0 if last2 is None else last2, r)
                last2 = r
                r = pltpu.roll(x, 4, 0)
                x = x + jnp.where(sub < 4, 0.0 if last4 is None else last4, r)
                last4 = r
                x16 = x if last8 is None else x + last8
                last8 = x
                x32 = x16 if len(last16) < 2 else x16 + last16[-2]
                last16 = last16[-1:] + [x16]
                x64 = x32 if len(last32) < 4 else x32 + last32[-4]
                last32 = last32[-3:] + [x32]
                if SKIP_GROUPS <= g < own_groups:
                    x64 = x64 * inverse[rows_of(g), lanes]
                    sums[0, f, g - SKIP_GROUPS] += folded(x64)
                    sums[1, f, g - SKIP_GROUPS] += folded(x64 * x64)
                    to, at = divmod(g - SKIP_GROUPS, main // 2)
                    (low, high)[to][f, rows_of(at), lanes] = x64
                else:
                    to = g if g < SKIP_GROUPS else g - main
                    edge[f, rows_of(to), lanes] = x64
            return carry

        lax.fori_loop(0, fields, one_field, 0)
        return carry

    lax.fori_loop(0, chunks, chunk, 0)
    for stat in range(2):
        for f in range(fields):
            for g in range(main):
                tiles[stat] = jnp.where(lane == f * main + g, total_of(sums[stat, f, g]), tiles[stat])
    for d in range(pay.shape[0]):
        pay[d, :GROUP, :] = tiles[0]
        pay[d, GROUP:, :] = tiles[1]


def spread_columns(tile, cols, spots):
    for i, spot in enumerate(spots):
        cols[i] = column(tile, spot, LANE)


def tiles_of(assets):
    return [pl.ds(at, LANE) for at in range(0, assets, LANE)]


def row_moments(source, mine, inverse, where, cs, ss):
    fields, _, assets = source.shape
    acc = [None] * (2 * fields)

    def added(i, x):
        acc[i] = x if acc[i] is None else acc[i] + x

    for lanes in tiles_of(assets):
        listed = inverse[where, lanes] > 0.0
        for f in range(fields):
            z = clipped_score(source[f, mine, lanes], cs[f], ss[f])
            z = jnp.where(listed, z, 0.0)
            added(f, z)
            added(fields + f, z * z)
    return acc


def group_rows(g):
    return pl.ds(pl.multiple_of(g * GROUP, GROUP), GROUP)


def second_pass(gathered, low, high, inverse, stats, part, centers, scales, sums):
    fields, _, assets = low.shape
    main = (inverse.shape[0] - LATE) // GROUP - SKIP_GROUPS
    first = fields * main
    total = summed(gathered)
    t0, t1 = total[:GROUP], total[GROUP:]
    lane = lanes_iota()
    present = t1
    for f in range(fields):
        moved = pltpu.roll(t0, (f * main - first) % LANE, 1)
        present = jnp.where((lane >= f * main) & (lane < (f + 1) * main), moved, present)
    present = jnp.maximum(present, 1.0)
    center, scale = moments(t0, t1, present)
    stats[0], stats[1], stats[2] = center, scale, present
    spread_columns(center, centers, range(first))
    spread_columns(scale, scales, range(first))

    half = main // 2
    for source, skip in ((low, 0), (high, half)):

        def group(i, carry):
            g = i + skip
            cs = [centers[f * main + g] for f in range(fields)]
            ss = [scales[f * main + g] for f in range(fields)]
            where = group_rows(g + SKIP_GROUPS)
            acc = row_moments(source, group_rows(i), inverse, where, cs, ss)
            for stat in range(2):
                for f in range(fields):
                    sums[stat, f * main + g] = acc[stat * fields + f]
            return carry

        lax.fori_loop(0, half, group, 0)
    for stat in range(2):
        tile = jnp.zeros((GROUP, LANE), jnp.float32)
        for spot in range(first):
            tile = jnp.where(lane == spot, total_of(sums[stat, spot]), tile)
        part[rows_of(stat), :] = tile


def late_first_pass(edge, tail, head, from_ref, inverse, part, late, whole, pay):
    fields, _, assets = edge.shape
    rows = inverse.shape[0] - LATE
    base, base_next = block_starts(rows)
    follows = jnp.where(base_next > 0, 1.0, 0.0)
    width = 4 * LANE
    sub = sublanes(width)
    lane = lanes_iota()
    first = LANE - 2 * fields * LATE_GROUPS
    tiles = [part[:GROUP, :], part[GROUP:, :]]
    for f in range(fields):

        def tile(i, acc):
            lanes = pl.ds(pl.multiple_of(i * width, width), width)
            age = sub - jnp.maximum(from_ref[:, lanes], 0)
            acc = list(acc)
            for side, ref, at in ((0, tail, base - LATE), (1, head, base_next)):
                start = age + at
                masked = [
                    jnp.where(start >= -g * GROUP, ref[f, rows_of(g), lanes], 0.0)
                    for g in range(LATE_GROUPS)
                ]
                running, last = prefix_groups(masked, width)
                if side == 0:
                    whole[f, :, lanes] = last
                for g in range(LATE_GROUPS):
                    if side == 0:
                        where = rows_of(LATE_GROUPS + g)
                        r = edge[f, where, lanes] + (last - running[g])
                    else:
                        where = rows_of(rows // GROUP + g)
                        start_rows = rows_of(SKIP_GROUPS + g)
                        r = edge[f, start_rows, lanes] * follows + running[g]
                    r = r * inverse[where, lanes]
                    late[f, rows_of(side * LATE_GROUPS + g), lanes] = r
                    k = side * LATE_GROUPS + g
                    acc[k] = acc[k] + folded(r)
                    acc[2 * LATE_GROUPS + k] = acc[2 * LATE_GROUPS + k] + folded(r * r)
            return tuple(acc)

        zero = jnp.zeros((GROUP, LANE), jnp.float32)
        acc = lax.fori_loop(0, assets // width, tile, (zero,) * (4 * LATE_GROUPS))
        for side in range(2):
            for g in range(LATE_GROUPS):
                spot = first + (side * fields + f) * LATE_GROUPS + g
                for stat in range(2):
                    value = total_of(acc[(stat * 2 + side) * LATE_GROUPS + g])
                    tiles[stat] = jnp.where(lane == spot, value, tiles[stat])
    for d in range(pay.shape[0]):
        pay[d, :GROUP, :] = tiles[0]
        pay[d, GROUP:, :] = tiles[1]


def packed(t):
    half = LANE // 2
    low = pltpu.roll(t, half, 1)
    lane = lax.broadcasted_iota(jnp.int32, (GROUP // 2, LANE), 1)
    return jnp.where(lane < half, low[: GROUP // 2], t[GROUP // 2 :])


def unpacked(p):
    return jnp.concatenate([pltpu.roll(p, LANE // 2, 1), p], axis=0)


def late_second_pass(gathered, stats, late, inverse, level, pay):
    fields, _, assets = late.shape
    rows = inverse.shape[0] - LATE
    total = summed(gathered)
    center, scale = moments(total[:GROUP], total[GROUP:], stats[2])
    level[0], level[1] = center, scale
    first = LANE - 2 * fields * LATE_GROUPS
    back = LANE - first
    lane = lanes_iota()
    out = jnp.zeros((GROUP, LANE), jnp.float32)
    for side in range(2):
        for g in range(LATE_GROUPS):
            spots = [first + (side * fields + f) * LATE_GROUPS + g for f in range(fields)]
            cs = [column(center, spot, LANE) for spot in spots]
            ss = [column(scale, spot, LANE) for spot in spots]
            where = rows_of(LATE_GROUPS + g if side == 0 else rows // GROUP + g)
            mine = rows_of(side * LATE_GROUPS + g)
            acc = row_moments(late, mine, inverse, where, cs, ss)
            for f in range(fields):
                out = jnp.where(lane == spots[f], total_of(acc[f]), out)
                out = jnp.where(lane == spots[f] - back, total_of(acc[fields + f]), out)
    out = packed(out)
    for d in range(pay.shape[0]):
        pay[d] = out


def final_rows(f, where, source, mine, inverse, stage, put, cols):
    c1, s1, c2, s2 = cols
    for lanes in tiles_of(source.shape[2]):
        z = (clipped_score(source[f, mine, lanes], c1, s1) - c2) * s2
        stage[f, put, lanes] = jnp.where(inverse[where, lanes] > 0.0, z, 0.0)


def send_pass(gathered, stats, level, level4, pay):
    total = unpacked(summed(gathered))
    back = 32
    square = pltpu.roll(total, back, 1)
    center, scale = moments(total, square, stats[2])
    level4[0], level4[1] = center, scale
    lane = lanes_iota()
    out = jnp.zeros((GROUP, LANE), jnp.float32)
    for i, t in enumerate((level[0], level[1], center, scale)):
        moved = pltpu.roll(t, 16 * (i + 1), 1)
        out = jnp.where((lane >= 16 * i) & (lane < 16 * (i + 1)), moved, out)
    pay[...] = out


def final_pass(
    edge, low, high, late, tail, whole, from_ref, inverse, centers, scales, level, level4,
    out, rolled, stage, sems,
):
    fields, rows, assets = out.shape
    main = rows // GROUP - SKIP_GROUPS
    first = LANE - 2 * fields * LATE_GROUPS
    late_tiles = (level[0], level[1], level4[0], level4[1])
    copies = []
    half = main // 2
    for f in range(fields):
        for g in range(LATE_GROUPS):
            spot = first + f * LATE_GROUPS + g
            column_set = [column(t, spot, LANE) for t in late_tiles]
            where = rows_of(LATE_GROUPS + g)
            final_rows(f, where, late, rows_of(g), inverse, stage, rows_of(g), column_set)
        for part in range(2):
            for g in range(part * half, (part + 1) * half):
                spot = f * main + g
                c2, s2 = column(level[0], spot, LANE), column(level[1], spot, LANE)
                where = rows_of(g + SKIP_GROUPS)
                put = rows_of(g + LATE_GROUPS)
                column_set = (centers[spot], scales[spot], c2, s2)
                source = (low, high)[part]
                mine = rows_of(g - part * half)
                final_rows(f, where, source, mine, inverse, stage, put, column_set)
            begin = part * (LATE_GROUPS + half) * GROUP
            size = (half + (LATE_GROUPS if part == 0 else 0)) * GROUP
            copy = pltpu.make_async_copy(
                stage.at[f, pl.ds(begin, size), :],
                out.at[f, pl.ds(LATE + begin, size), :],
                sems.at[2 * f + part],
            )
            copy.start()
            copies.append(copy)
    base = block_starts(rows)[0]
    width = 4 * LANE
    sub = sublanes(width)
    for f in range(fields):

        def tile(i, carry):
            lanes = pl.ds(pl.multiple_of(i * width, width), width)
            start = sub - jnp.maximum(from_ref[:, lanes], 0) + (base - WINDOW)
            masked = [
                jnp.where(start >= -g * GROUP, tail[f, rows_of(g), lanes], 0.0)
                for g in range(LATE_GROUPS)
            ]
            running, last = prefix_groups(masked, width)
            last = last + whole[f, :, lanes]
            for g in range(LATE_GROUPS):
                r = edge[f, rows_of(g), lanes] + (last - running[g])
                rolled[f, rows_of(g), lanes] = r * inverse[rows_of(g), lanes]
            return carry

        lax.fori_loop(0, assets // width, tile, 0)
    for copy in copies:
        copy.wait()


def head_final_pass(rolled, inverse, sent, prior, out, stage, sems):
    fields, _, assets = rolled.shape
    levels = sent[...]
    copies = []
    for f in range(fields):
        for g in range(LATE_GROUPS):
            cols = [column(levels, 16 * i + f * LATE_GROUPS + g, LANE) for i in range(4)]
            rows = rows_of(g)
            final_rows(f, rows, rolled, rows, inverse, stage, rows, cols)
        copy = pltpu.make_async_copy(stage.at[f], out.at[f, pl.ds(0, LATE), :], sems.at[f])
        copy.start()
        copies.append(copy)
    for copy in copies:
        copy.wait()


def shape(*dims):
    return jax.ShapeDtypeStruct(dims, jnp.float32)


def call(body, name, ins, outs, out_specs, scratch=(), limit=8, flops=0, aliases=None):
    return pl.pallas_call(
        body,
        name=name,
        out_shape=outs,
        in_specs=ins,
        out_specs=out_specs,
        scratch_shapes=list(scratch),
        input_output_aliases=aliases or {},
        compiler_params=pltpu.CompilerParams(vmem_limit_bytes=limit * MIB),
        cost_estimate=pl.CostEstimate(flops=flops, bytes_accessed=0, transcendentals=0),
    )


def per_device(values, listed_from, listed_until):
    fields, rows, assets = values.shape
    n = lax.axis_size("asset")
    blocks = lax.axis_size("tm")
    ring = [(i, (i + 1) % blocks) for i in range(blocks)]
    back = [((i + 1) % blocks, i) for i in range(blocks)]
    work = fields * rows * assets
    slab = shape(fields, LATE, assets)
    near, head = call(
        cut, "cut", [HBM], (slab, slab), (VMEM, VMEM), [pltpu.SemaphoreType.DMA((2,))],
        limit=44,
    )(values)
    tail_near = lax.ppermute(near, "tm", ring)
    head = lax.ppermute(head, "tm", back)
    opened, closed = listed_from.reshape(1, assets), listed_until.reshape(1, assets)
    main = rows // GROUP - SKIP_GROUPS
    tile = shape(GROUP, LANE)
    pair = shape(2, GROUP, LANE)
    exchange = functools.partial(
        lax.all_to_all, axis_name="asset", split_axis=0, concat_axis=0, tiled=True
    )

    width = 2 * LANE
    chunks = assets // width
    half = shape(fields, (rows - WINDOW) // 2, assets)
    edge, low, high, inverse, pay, far = call(
        first_pass, "first_pass", [HBM] * 3,
        (
            shape(fields, WINDOW + LATE, assets), half, half,
            shape(rows + LATE, assets), shape(n, 2 * GROUP, LANE), slab,
        ),
        (VMEM,) * 6,
        [
            pltpu.VMEM((1, assets), jnp.int32),
            pltpu.VMEM((1, assets), jnp.int32),
            pltpu.VMEM((chunks, fields, rows, width), jnp.float32),
            pltpu.VMEM((2, fields, main, GROUP, LANE), jnp.float32),
            pltpu.SemaphoreType.DMA((chunks,)),
            pltpu.SemaphoreType.DMA((2,)),
        ],
        limit=40, flops=20 * work,
    )(values, opened, closed)
    tail_far = lax.ppermute(far, "tm", ring)
    gathered = exchange(pay)
    columns = shape(fields * main, GROUP, LANE)
    stats, part, centers, scales = call(
        second_pass, "second_pass", [VMEM] * 4,
        (shape(3, GROUP, LANE), shape(2 * GROUP, LANE), columns, columns), (VMEM,) * 4,
        [pltpu.VMEM((2, fields * main, GROUP, LANE), jnp.float32)], limit=16, flops=10 * work,
    )(gathered, low, high, inverse)
    late, whole, pay = call(
        late_first_pass, "late_first_pass", [VMEM] * 6,
        (shape(fields, 2 * LATE, assets), shape(fields, GROUP, assets), shape(n, 2 * GROUP, LANE)),
        (VMEM, VMEM, VMEM), limit=20, flops=5 * work,
    )(edge, tail_near, head, opened, inverse, part)
    gathered = exchange(pay)
    level, pay = call(
        late_second_pass, "late_second_pass", [VMEM] * 4,
        (pair, shape(n, GROUP // 2, LANE)), (VMEM, VMEM), limit=16, flops=3 * work,
    )(gathered, stats, late, inverse)
    gathered = exchange(pay)
    level4, pay = call(
        send_pass, "send_pass", [VMEM] * 3, (pair, tile), (VMEM, VMEM), flops=work // 100,
    )(gathered, stats, level)
    sent = lax.ppermute(pay, "tm", ring)
    out, rolled = call(
        final_pass, "final_pass", [VMEM] * 12,
        (shape(fields, rows, assets), slab), (HBM, VMEM),
        [
            pltpu.VMEM((fields, rows - LATE, assets), jnp.float32),
            pltpu.SemaphoreType.DMA((2 * fields,)),
        ],
        limit=16, flops=10 * work,
    )(edge, low, high, late, tail_far, whole, opened, inverse, centers, scales, level, level4)
    return call(
        head_final_pass, "head_final_pass", [VMEM] * 3 + [HBM],
        shape(fields, rows, assets), HBM,
        [pltpu.VMEM((fields, LATE, assets), jnp.float32), pltpu.SemaphoreType.DMA((fields,))],
        limit=16, flops=2 * work, aliases={3: 0},
    )(rolled, inverse, sent, out)


def solution(mesh):
    in_specs = (P(None, "tm", "asset"), P("asset"), P("asset"))
    out_specs = P(None, "tm", "asset")
    return jax.shard_map(
        per_device, mesh=mesh, in_specs=in_specs, out_specs=out_specs, check_vma=False
    )
```

```python
import functools

import jax
import jax.numpy as jnp
from jax import lax
from jax.experimental import pallas as pl
from jax.experimental.pallas import tpu as pltpu
from jax.sharding import PartitionSpec as P

WINDOW = 64
EPS = 0.1
LIMIT = 3.0
GROUP = 8
LANE = 128
LATE = 32
LATE_GROUPS = LATE // GROUP
SKIP_GROUPS = WINDOW // GROUP
VMEM = pl.BlockSpec(memory_space=pltpu.VMEM)
HBM = pl.BlockSpec(memory_space=pltpu.HBM)
MIB = 1 << 20


def rows_of(g):
    return pl.ds(g * GROUP, GROUP)


def block_starts(rows):
    block, blocks = lax.axis_index("tm"), lax.axis_size("tm")
    return block * rows, lax.rem(block + 1, blocks) * rows


def sublanes(width):
    return lax.broadcasted_iota(jnp.int32, (GROUP, width), 0)


def lanes_iota():
    return lax.broadcasted_iota(jnp.int32, (GROUP, LANE), 1)


def folded(x):
    total = x[:, :LANE]
    for at in range(LANE, x.shape[1], LANE):
        total = total + x[:, at : at + LANE]
    return total


def total_of(x):
    return jnp.sum(x, axis=1, keepdims=True)


def column(tile, lane, width):
    return jnp.broadcast_to(tile[:, lane : lane + 1], (GROUP, width))


def clipped_score(x, center, scale):
    return jnp.minimum(jnp.maximum((x - center) * scale, -LIMIT), LIMIT)


def moments(total, square, present):
    center = total / present
    spread = jnp.maximum(square / present - center * center, 0.0)
    return center, 1.0 / jnp.sqrt(spread + EPS)


def summed(gathered):
    total = gathered[0]
    for d in range(1, gathered.shape[0]):
        total = total + gathered[d]
    return total


def prefix_groups(groups, width):
    sub = sublanes(width)
    carried, out = None, []
    for x in groups:
        for s in (1, 2, 4):
            x = x + jnp.where(sub < s, 0.0, pltpu.roll(x, s, 0))
        if carried is not None:
            x = x + carried
        carried = jnp.broadcast_to(x[GROUP - 1 :, :], (GROUP, width))
        out.append(x)
    return out, carried


def cut(x_hbm, near, head, sems):
    rows = x_hbm.shape[1]
    copies = [
        pltpu.make_async_copy(x_hbm.at[:, pl.ds(rows - LATE, LATE), :], near, sems.at[0]),
        pltpu.make_async_copy(x_hbm.at[:, pl.ds(0, LATE), :], head, sems.at[1]),
    ]
    for copy in copies:
        copy.start()
    for copy in copies:
        copy.wait()


def first_pass(
    x_hbm, from_hbm, until_hbm,
    edge, low, high, inverse, pay, far, from_ref, until_ref, xs, sums, sems, date_sems,
):
    fields, rows, assets = x_hbm.shape
    own_groups = rows // GROUP
    groups = own_groups + LATE_GROUPS
    main = own_groups - SKIP_GROUPS
    base, base_next = block_starts(rows)
    chunks, _, _, width = xs.shape

    def fetch(c):
        lanes = pl.ds(pl.multiple_of(c * width, width), width)
        return pltpu.make_async_copy(x_hbm.at[:, :, lanes], xs.at[c], sems.at[c])

    dates = [
        pltpu.make_async_copy(from_hbm, from_ref, date_sems.at[0]),
        pltpu.make_async_copy(until_hbm, until_ref, date_sems.at[1]),
    ]
    for copy in dates:
        copy.start()
    for c in range(chunks):
        fetch(c).start()
    sums[...] = jnp.zeros_like(sums)
    wide = 4 * LANE
    sub = sublanes(wide)
    lane = lanes_iota()
    first = fields * main
    tiles = [jnp.zeros((GROUP, LANE), jnp.float32) for _ in range(2)]
    for copy in dates:
        copy.wait()
    for g in range(groups):
        at = base + g * GROUP if g < own_groups else base_next + (g - own_groups) * GROUP
        count = jnp.zeros((GROUP, LANE), jnp.float32)
        for start in range(0, assets, wide):
            lanes = pl.ds(start, wide)
            seen = sub - jnp.maximum(from_ref[:, lanes], 0) + at
            listed = (seen >= 0) & (until_ref[:, lanes] - sub > at)
            counted = jnp.clip(seen + 1, 1, WINDOW).astype(jnp.float32)
            inverse[rows_of(g), lanes] = jnp.where(listed, 1.0 / counted, 0.0)
            count = count + folded(jnp.where(listed, 1.0, 0.0))
        if SKIP_GROUPS <= g < own_groups:
            tiles[0] = jnp.where(lane == first + g - SKIP_GROUPS, total_of(count), tiles[0])
        elif g >= SKIP_GROUPS - LATE_GROUPS:
            side = 0 if g < SKIP_GROUPS else 1
            k = g - LATE_GROUPS if side == 0 else g - own_groups
            spot = lane - (first + side * fields * LATE_GROUPS)
            here = (spot >= 0) & (spot < fields * LATE_GROUPS) & (lax.rem(spot, LATE_GROUPS) == k)
            tiles[1] = jnp.where(here, total_of(count), tiles[1])
    sub = sublanes(width)

    def chunk(c, carry):
        lanes = pl.ds(pl.multiple_of(c * width, width), width)
        start = base + sub - jnp.maximum(from_ref[:, lanes], 0)
        fetch(c).wait()

        def one_field(f, carry):
            last1 = last2 = last4 = last8 = None
            last16, last32 = [], []
            for g in range(groups):
                if own_groups - SKIP_GROUPS <= g < own_groups - LATE_GROUPS:
                    to = rows_of(g - (own_groups - SKIP_GROUPS))
                    far[f, to, lanes] = xs[c, f, rows_of(g), :]
                if g < own_groups:
                    x = jnp.where(start >= -g * GROUP, xs[c, f, rows_of(g), :], 0.0)
                else:
                    x = jnp.zeros((GROUP, width), jnp.float32)
                r = pltpu.roll(x, 1, 0)
                x = x + jnp.where(sub < 1, 0.0 if last1 is None else last1, r)
                last1 = r
                r = pltpu.roll(x, 2, 0)
                x = x + jnp.where(sub < 2, 0.0 if last2 is None else last2, r)
                last2 = r
                r = pltpu.roll(x, 4, 0)
                x = x + jnp.where(sub < 4, 0.0 if last4 is None else last4, r)
                last4 = r
                x16 = x if last8 is None else x + last8
                last8 = x
                x32 = x16 if len(last16) < 2 else x16 + last16[-2]
                last16 = last16[-1:] + [x16]
                x64 = x32 if len(last32) < 4 else x32 + last32[-4]
                last32 = last32[-3:] + [x32]
                if SKIP_GROUPS <= g < own_groups:
                    x64 = x64 * inverse[rows_of(g), lanes]
                    sums[0, f, g - SKIP_GROUPS] += folded(x64)
                    sums[1, f, g - SKIP_GROUPS] += folded(x64 * x64)
                    to, at = divmod(g - SKIP_GROUPS, main // 2)
                    (low, high)[to][f, rows_of(at), lanes] = x64
                else:
                    to = g if g < SKIP_GROUPS else g - main
                    edge[f, rows_of(to), lanes] = x64
            return carry

        lax.fori_loop(0, fields, one_field, 0)
        return carry

    lax.fori_loop(0, chunks, chunk, 0)
    for stat in range(2):
        for f in range(fields):
            for g in range(main):
                tiles[stat] = jnp.where(lane == f * main + g, total_of(sums[stat, f, g]), tiles[stat])
    for d in range(pay.shape[0]):
        pay[d, :GROUP, :] = tiles[0]
        pay[d, GROUP:, :] = tiles[1]


def spread_columns(tile, cols, spots):
    for i, spot in enumerate(spots):
        cols[i] = column(tile, spot, LANE)


def tiles_of(assets):
    return [pl.ds(at, LANE) for at in range(0, assets, LANE)]


def row_moments(source, mine, inverse, where, cs, ss):
    fields, _, assets = source.shape
    acc = [None] * (2 * fields)

    def added(i, x):
        acc[i] = x if acc[i] is None else acc[i] + x

    for lanes in tiles_of(assets):
        listed = inverse[where, lanes] > 0.0
        for f in range(fields):
            z = clipped_score(source[f, mine, lanes], cs[f], ss[f])
            z = jnp.where(listed, z, 0.0)
            added(f, z)
            added(fields + f, z * z)
    return acc


def group_rows(g):
    return pl.ds(pl.multiple_of(g * GROUP, GROUP), GROUP)


def second_pass(gathered, low, high, inverse, stats, part, centers, scales, sums):
    fields, _, assets = low.shape
    main = (inverse.shape[0] - LATE) // GROUP - SKIP_GROUPS
    first = fields * main
    total = summed(gathered)
    t0, t1 = total[:GROUP], total[GROUP:]
    lane = lanes_iota()
    present = t1
    for f in range(fields):
        moved = pltpu.roll(t0, (f * main - first) % LANE, 1)
        present = jnp.where((lane >= f * main) & (lane < (f + 1) * main), moved, present)
    present = jnp.maximum(present, 1.0)
    center, scale = moments(t0, t1, present)
    stats[0], stats[1], stats[2] = center, scale, present
    spread_columns(center, centers, range(first))
    spread_columns(scale, scales, range(first))

    half = main // 2
    for source, skip in ((low, 0), (high, half)):

        def group(i, carry):
            g = i + skip
            cs = [centers[f * main + g] for f in range(fields)]
            ss = [scales[f * main + g] for f in range(fields)]
            where = group_rows(g + SKIP_GROUPS)
            acc = row_moments(source, group_rows(i), inverse, where, cs, ss)
            for stat in range(2):
                for f in range(fields):
                    sums[stat, f * main + g] = acc[stat * fields + f]
            return carry

        lax.fori_loop(0, half, group, 0)
    for stat in range(2):
        tile = jnp.zeros((GROUP, LANE), jnp.float32)
        for spot in range(first):
            tile = jnp.where(lane == spot, total_of(sums[stat, spot]), tile)
        part[rows_of(stat), :] = tile


def late_first_pass(edge, tail, head, from_ref, inverse, part, late, whole, pay):
    fields, _, assets = edge.shape
    rows = inverse.shape[0] - LATE
    base, base_next = block_starts(rows)
    follows = jnp.where(base_next > 0, 1.0, 0.0)
    width = 4 * LANE
    sub = sublanes(width)
    lane = lanes_iota()
    first = LANE - 2 * fields * LATE_GROUPS
    tiles = [part[:GROUP, :], part[GROUP:, :]]
    for f in range(fields):

        def tile(i, acc):
            lanes = pl.ds(pl.multiple_of(i * width, width), width)
            age = sub - jnp.maximum(from_ref[:, lanes], 0)
            acc = list(acc)
            for side, ref, at in ((0, tail, base - LATE), (1, head, base_next)):
                start = age + at
                masked = [
                    jnp.where(start >= -g * GROUP, ref[f, rows_of(g), lanes], 0.0)
                    for g in range(LATE_GROUPS)
                ]
                running, last = prefix_groups(masked, width)
                if side == 0:
                    whole[f, :, lanes] = last
                for g in range(LATE_GROUPS):
                    if side == 0:
                        where = rows_of(LATE_GROUPS + g)
                        r = edge[f, where, lanes] + (last - running[g])
                    else:
                        where = rows_of(rows // GROUP + g)
                        start_rows = rows_of(SKIP_GROUPS + g)
                        r = edge[f, start_rows, lanes] * follows + running[g]
                    r = r * inverse[where, lanes]
                    late[f, rows_of(side * LATE_GROUPS + g), lanes] = r
                    k = side * LATE_GROUPS + g
                    acc[k] = acc[k] + folded(r)
                    acc[2 * LATE_GROUPS + k] = acc[2 * LATE_GROUPS + k] + folded(r * r)
            return tuple(acc)

        zero = jnp.zeros((GROUP, LANE), jnp.float32)
        acc = lax.fori_loop(0, assets // width, tile, (zero,) * (4 * LATE_GROUPS))
        for side in range(2):
            for g in range(LATE_GROUPS):
                spot = first + (side * fields + f) * LATE_GROUPS + g
                for stat in range(2):
                    value = total_of(acc[(stat * 2 + side) * LATE_GROUPS + g])
                    tiles[stat] = jnp.where(lane == spot, value, tiles[stat])
    for d in range(pay.shape[0]):
        pay[d, :GROUP, :] = tiles[0]
        pay[d, GROUP:, :] = tiles[1]


def packed(t):
    half = LANE // 2
    low = pltpu.roll(t, half, 1)
    lane = lax.broadcasted_iota(jnp.int32, (GROUP // 2, LANE), 1)
    return jnp.where(lane < half, low[: GROUP // 2], t[GROUP // 2 :])


def unpacked(p):
    return jnp.concatenate([pltpu.roll(p, LANE // 2, 1), p], axis=0)


def late_second_pass(gathered, stats, late, inverse, level, pay):
    fields, _, assets = late.shape
    rows = inverse.shape[0] - LATE
    total = summed(gathered)
    center, scale = moments(total[:GROUP], total[GROUP:], stats[2])
    level[0], level[1] = center, scale
    first = LANE - 2 * fields * LATE_GROUPS
    back = LANE - first
    lane = lanes_iota()
    out = jnp.zeros((GROUP, LANE), jnp.float32)
    for side in range(2):
        for g in range(LATE_GROUPS):
            spots = [first + (side * fields + f) * LATE_GROUPS + g for f in range(fields)]
            cs = [column(center, spot, LANE) for spot in spots]
            ss = [column(scale, spot, LANE) for spot in spots]
            where = rows_of(LATE_GROUPS + g if side == 0 else rows // GROUP + g)
            mine = rows_of(side * LATE_GROUPS + g)
            acc = row_moments(late, mine, inverse, where, cs, ss)
            for f in range(fields):
                out = jnp.where(lane == spots[f], total_of(acc[f]), out)
                out = jnp.where(lane == spots[f] - back, total_of(acc[fields + f]), out)
    out = packed(out)
    for d in range(pay.shape[0]):
        pay[d] = out


def final_rows(f, where, source, mine, inverse, stage, put, cols):
    c1, s1, c2, s2 = cols
    for lanes in tiles_of(source.shape[2]):
        z = (clipped_score(source[f, mine, lanes], c1, s1) - c2) * s2
        stage[f, put, lanes] = jnp.where(inverse[where, lanes] > 0.0, z, 0.0)


def send_pass(gathered, stats, level, level4, pay):
    total = unpacked(summed(gathered))
    back = 32
    square = pltpu.roll(total, back, 1)
    center, scale = moments(total, square, stats[2])
    level4[0], level4[1] = center, scale
    lane = lanes_iota()
    out = jnp.zeros((GROUP, LANE), jnp.float32)
    for i, t in enumerate((level[0], level[1], center, scale)):
        moved = pltpu.roll(t, 16 * (i + 1), 1)
        out = jnp.where((lane >= 16 * i) & (lane < 16 * (i + 1)), moved, out)
    pay[...] = out


def final_pass(
    edge, low, high, late, tail, whole, from_ref, inverse, centers, scales, level, level4,
    out, rolled, stage, sems,
):
    fields, rows, assets = out.shape
    main = rows // GROUP - SKIP_GROUPS
    first = LANE - 2 * fields * LATE_GROUPS
    late_tiles = (level[0], level[1], level4[0], level4[1])
    copies = []
    half = main // 2
    for f in range(fields):
        for g in range(LATE_GROUPS):
            spot = first + f * LATE_GROUPS + g
            column_set = [column(t, spot, LANE) for t in late_tiles]
            where = rows_of(LATE_GROUPS + g)
            final_rows(f, where, late, rows_of(g), inverse, stage, rows_of(g), column_set)
        for part in range(2):
            for g in range(part * half, (part + 1) * half):
                spot = f * main + g
                c2, s2 = column(level[0], spot, LANE), column(level[1], spot, LANE)
                where = rows_of(g + SKIP_GROUPS)
                put = rows_of(g + LATE_GROUPS)
                column_set = (centers[spot], scales[spot], c2, s2)
                source = (low, high)[part]
                mine = rows_of(g - part * half)
                final_rows(f, where, source, mine, inverse, stage, put, column_set)
            begin = part * (LATE_GROUPS + half) * GROUP
            size = (half + (LATE_GROUPS if part == 0 else 0)) * GROUP
            copy = pltpu.make_async_copy(
                stage.at[f, pl.ds(begin, size), :],
                out.at[f, pl.ds(LATE + begin, size), :],
                sems.at[2 * f + part],
            )
            copy.start()
            copies.append(copy)
    base = block_starts(rows)[0]
    width = 4 * LANE
    sub = sublanes(width)
    for f in range(fields):

        def tile(i, carry):
            lanes = pl.ds(pl.multiple_of(i * width, width), width)
            start = sub - jnp.maximum(from_ref[:, lanes], 0) + (base - WINDOW)
            masked = [
                jnp.where(start >= -g * GROUP, tail[f, rows_of(g), lanes], 0.0)
                for g in range(LATE_GROUPS)
            ]
            running, last = prefix_groups(masked, width)
            last = last + whole[f, :, lanes]
            for g in range(LATE_GROUPS):
                r = edge[f, rows_of(g), lanes] + (last - running[g])
                rolled[f, rows_of(g), lanes] = r * inverse[rows_of(g), lanes]
            return carry

        lax.fori_loop(0, assets // width, tile, 0)
    for copy in copies:
        copy.wait()


def head_final_pass(rolled, inverse, sent, prior, out, stage, sems):
    fields, _, assets = rolled.shape
    levels = sent[...]
    copies = []
    for f in range(fields):
        for g in range(LATE_GROUPS):
            cols = [column(levels, 16 * i + f * LATE_GROUPS + g, LANE) for i in range(4)]
            rows = rows_of(g)
            final_rows(f, rows, rolled, rows, inverse, stage, rows, cols)
        copy = pltpu.make_async_copy(stage.at[f], out.at[f, pl.ds(0, LATE), :], sems.at[f])
        copy.start()
        copies.append(copy)
    for copy in copies:
        copy.wait()


def shape(*dims):
    return jax.ShapeDtypeStruct(dims, jnp.float32)


def call(body, name, ins, outs, out_specs, scratch=(), limit=8, flops=0, aliases=None):
    return pl.pallas_call(
        body,
        name=name,
        out_shape=outs,
        in_specs=ins,
        out_specs=out_specs,
        scratch_shapes=list(scratch),
        input_output_aliases=aliases or {},
        compiler_params=pltpu.CompilerParams(vmem_limit_bytes=limit * MIB),
        cost_estimate=pl.CostEstimate(flops=flops, bytes_accessed=0, transcendentals=0),
    )


def per_device(values, listed_from, listed_until):
    fields, rows, assets = values.shape
    n = lax.axis_size("asset")
    blocks = lax.axis_size("tm")
    ring = [(i, (i + 1) % blocks) for i in range(blocks)]
    back = [((i + 1) % blocks, i) for i in range(blocks)]
    work = fields * rows * assets
    slab = shape(fields, LATE, assets)
    near, head = call(
        cut, "cut", [HBM], (slab, slab), (VMEM, VMEM), [pltpu.SemaphoreType.DMA((2,))],
        limit=44,
    )(values)
    tail_near = lax.ppermute(near, "tm", ring)
    head = lax.ppermute(head, "tm", back)
    opened, closed = listed_from.reshape(1, assets), listed_until.reshape(1, assets)
    main = rows // GROUP - SKIP_GROUPS
    tile = shape(GROUP, LANE)
    pair = shape(2, GROUP, LANE)
    exchange = functools.partial(
        lax.all_to_all, axis_name="asset", split_axis=0, concat_axis=0, tiled=True
    )

    width = 2 * LANE
    chunks = assets // width
    half = shape(fields, (rows - WINDOW) // 2, assets)
    edge, low, high, inverse, pay, far = call(
        first_pass, "first_pass", [HBM] * 3,
        (
            shape(fields, WINDOW + LATE, assets), half, half,
            shape(rows + LATE, assets), shape(n, 2 * GROUP, LANE), slab,
        ),
        (VMEM,) * 6,
        [
            pltpu.VMEM((1, assets), jnp.int32),
            pltpu.VMEM((1, assets), jnp.int32),
            pltpu.VMEM((chunks, fields, rows, width), jnp.float32),
            pltpu.VMEM((2, fields, main, GROUP, LANE), jnp.float32),
            pltpu.SemaphoreType.DMA((chunks,)),
            pltpu.SemaphoreType.DMA((2,)),
        ],
        limit=40, flops=20 * work,
    )(values, opened, closed)
    gathered = exchange(pay)
    columns = shape(fields * main, GROUP, LANE)
    stats, part, centers, scales = call(
        second_pass, "second_pass", [VMEM] * 4,
        (shape(3, GROUP, LANE), shape(2 * GROUP, LANE), columns, columns), (VMEM,) * 4,
        [pltpu.VMEM((2, fields * main, GROUP, LANE), jnp.float32)], limit=16, flops=10 * work,
    )(gathered, low, high, inverse)
    far, part = lax.optimization_barrier((far, part))
    tail_far = lax.ppermute(far, "tm", ring)
    late, whole, pay = call(
        late_first_pass, "late_first_pass", [VMEM] * 6,
        (shape(fields, 2 * LATE, assets), shape(fields, GROUP, assets), shape(n, 2 * GROUP, LANE)),
        (VMEM, VMEM, VMEM), limit=20, flops=5 * work,
    )(edge, tail_near, head, opened, inverse, part)
    gathered = exchange(pay)
    level, pay = call(
        late_second_pass, "late_second_pass", [VMEM] * 4,
        (pair, shape(n, GROUP // 2, LANE)), (VMEM, VMEM), limit=16, flops=3 * work,
    )(gathered, stats, late, inverse)
    gathered = exchange(pay)
    level4, pay = call(
        send_pass, "send_pass", [VMEM] * 3, (pair, tile), (VMEM, VMEM), flops=work // 100,
    )(gathered, stats, level)
    sent = lax.ppermute(pay, "tm", ring)
    out, rolled = call(
        final_pass, "final_pass", [VMEM] * 12,
        (shape(fields, rows, assets), slab), (HBM, VMEM),
        [
            pltpu.VMEM((fields, rows - LATE, assets), jnp.float32),
            pltpu.SemaphoreType.DMA((2 * fields,)),
        ],
        limit=16, flops=10 * work,
    )(edge, low, high, late, tail_far, whole, opened, inverse, centers, scales, level, level4)
    return call(
        head_final_pass, "head_final_pass", [VMEM] * 3 + [HBM],
        shape(fields, rows, assets), HBM,
        [pltpu.VMEM((fields, LATE, assets), jnp.float32), pltpu.SemaphoreType.DMA((fields,))],
        limit=16, flops=2 * work, aliases={3: 0},
    )(rolled, inverse, sent, out)


def solution(mesh):
    in_specs = (P(None, "tm", "asset"), P("asset"), P("asset"))
    out_specs = P(None, "tm", "asset")
    return jax.shard_map(
        per_device, mesh=mesh, in_specs=in_specs, out_specs=out_specs, check_vma=False
    )
```

```python
import functools

import jax
import jax.numpy as jnp
from jax import lax
from jax.experimental import pallas as pl
from jax.experimental.pallas import tpu as pltpu
from jax.sharding import PartitionSpec as P

WINDOW = 64
EPS = 0.1
LIMIT = 3.0
GROUP = 8
LANE = 128
LATE = 32
LATE_GROUPS = LATE // GROUP
SKIP_GROUPS = WINDOW // GROUP
VMEM = pl.BlockSpec(memory_space=pltpu.VMEM)
HBM = pl.BlockSpec(memory_space=pltpu.HBM)
MIB = 1 << 20


def rows_of(g):
    return pl.ds(g * GROUP, GROUP)


def block_starts(rows):
    block, blocks = lax.axis_index("tm"), lax.axis_size("tm")
    return block * rows, lax.rem(block + 1, blocks) * rows


def sublanes(width):
    return lax.broadcasted_iota(jnp.int32, (GROUP, width), 0)


def lanes_iota():
    return lax.broadcasted_iota(jnp.int32, (GROUP, LANE), 1)


def folded(x):
    total = x[:, :LANE]
    for at in range(LANE, x.shape[1], LANE):
        total = total + x[:, at : at + LANE]
    return total


def total_of(x):
    return jnp.sum(x, axis=1, keepdims=True)


def column(tile, lane, width):
    return jnp.broadcast_to(tile[:, lane : lane + 1], (GROUP, width))


def clipped_score(x, center, scale):
    return jnp.minimum(jnp.maximum((x - center) * scale, -LIMIT), LIMIT)


def moments(total, square, present):
    center = total / present
    spread = jnp.maximum(square / present - center * center, 0.0)
    return center, 1.0 / jnp.sqrt(spread + EPS)


def summed(gathered):
    total = gathered[0]
    for d in range(1, gathered.shape[0]):
        total = total + gathered[d]
    return total


def prefix_groups(groups, width):
    sub = sublanes(width)
    carried, out = None, []
    for x in groups:
        for s in (1, 2, 4):
            x = x + jnp.where(sub < s, 0.0, pltpu.roll(x, s, 0))
        if carried is not None:
            x = x + carried
        carried = jnp.broadcast_to(x[GROUP - 1 :, :], (GROUP, width))
        out.append(x)
    return out, carried


def cut(x_hbm, near, head, sems):
    rows = x_hbm.shape[1]
    copies = [
        pltpu.make_async_copy(x_hbm.at[:, pl.ds(rows - LATE, LATE), :], near, sems.at[0]),
        pltpu.make_async_copy(x_hbm.at[:, pl.ds(0, LATE), :], head, sems.at[1]),
    ]
    for copy in copies:
        copy.start()
    for copy in copies:
        copy.wait()


def first_pass(
    x_hbm, from_hbm, until_hbm,
    edge, low, high, inverse, pay, far, from_ref, until_ref, xs, sums, sems, date_sems,
):
    fields, rows, assets = x_hbm.shape
    own_groups = rows // GROUP
    groups = own_groups + LATE_GROUPS
    main = own_groups - SKIP_GROUPS
    base, base_next = block_starts(rows)
    chunks, _, _, width = xs.shape

    def fetch(c):
        lanes = pl.ds(pl.multiple_of(c * width, width), width)
        return pltpu.make_async_copy(x_hbm.at[:, :, lanes], xs.at[c], sems.at[c])

    dates = [
        pltpu.make_async_copy(from_hbm, from_ref, date_sems.at[0]),
        pltpu.make_async_copy(until_hbm, until_ref, date_sems.at[1]),
    ]
    for copy in dates:
        copy.start()
    for c in range(chunks):
        fetch(c).start()
    sums[...] = jnp.zeros_like(sums)
    wide = 4 * LANE
    sub = sublanes(wide)
    lane = lanes_iota()
    first = fields * main
    tiles = [jnp.zeros((GROUP, LANE), jnp.float32) for _ in range(2)]
    for copy in dates:
        copy.wait()
    for g in range(groups):
        at = base + g * GROUP if g < own_groups else base_next + (g - own_groups) * GROUP
        count = jnp.zeros((GROUP, LANE), jnp.float32)
        for start in range(0, assets, wide):
            lanes = pl.ds(start, wide)
            seen = sub - jnp.maximum(from_ref[:, lanes], 0) + at
            listed = (seen >= 0) & (until_ref[:, lanes] - sub > at)
            counted = jnp.clip(seen + 1, 1, WINDOW).astype(jnp.float32)
            inverse[rows_of(g), lanes] = jnp.where(listed, 1.0 / counted, 0.0)
            count = count + folded(jnp.where(listed, 1.0, 0.0))
        if SKIP_GROUPS <= g < own_groups:
            tiles[0] = jnp.where(lane == first + g - SKIP_GROUPS, total_of(count), tiles[0])
        elif g >= SKIP_GROUPS - LATE_GROUPS:
            side = 0 if g < SKIP_GROUPS else 1
            k = g - LATE_GROUPS if side == 0 else g - own_groups
            spot = lane - (first + side * fields * LATE_GROUPS)
            here = (spot >= 0) & (spot < fields * LATE_GROUPS) & (lax.rem(spot, LATE_GROUPS) == k)
            tiles[1] = jnp.where(here, total_of(count), tiles[1])
    sub = sublanes(width)

    def chunk(c, carry):
        lanes = pl.ds(pl.multiple_of(c * width, width), width)
        start = base + sub - jnp.maximum(from_ref[:, lanes], 0)
        fetch(c).wait()

        def one_field(f, carry):
            last1 = last2 = last4 = last8 = None
            last16, last32 = [], []
            for g in range(groups):
                if own_groups - SKIP_GROUPS <= g < own_groups - LATE_GROUPS:
                    to = rows_of(g - (own_groups - SKIP_GROUPS))
                    far[f, to, lanes] = xs[c, f, rows_of(g), :]
                if g < own_groups:
                    x = jnp.where(start >= -g * GROUP, xs[c, f, rows_of(g), :], 0.0)
                else:
                    x = jnp.zeros((GROUP, width), jnp.float32)
                r = pltpu.roll(x, 1, 0)
                x = x + jnp.where(sub < 1, 0.0 if last1 is None else last1, r)
                last1 = r
                r = pltpu.roll(x, 2, 0)
                x = x + jnp.where(sub < 2, 0.0 if last2 is None else last2, r)
                last2 = r
                r = pltpu.roll(x, 4, 0)
                x = x + jnp.where(sub < 4, 0.0 if last4 is None else last4, r)
                last4 = r
                x16 = x if last8 is None else x + last8
                last8 = x
                x32 = x16 if len(last16) < 2 else x16 + last16[-2]
                last16 = last16[-1:] + [x16]
                x64 = x32 if len(last32) < 4 else x32 + last32[-4]
                last32 = last32[-3:] + [x32]
                if SKIP_GROUPS <= g < own_groups:
                    x64 = x64 * inverse[rows_of(g), lanes]
                    sums[0, f, g - SKIP_GROUPS] += folded(x64)
                    sums[1, f, g - SKIP_GROUPS] += folded(x64 * x64)
                    to, at = divmod(g - SKIP_GROUPS, main // 2)
                    (low, high)[to][f, rows_of(at), lanes] = x64
                else:
                    to = g if g < SKIP_GROUPS else g - main
                    edge[f, rows_of(to), lanes] = x64
            return carry

        lax.fori_loop(0, fields, one_field, 0)
        return carry

    lax.fori_loop(0, chunks, chunk, 0)
    for stat in range(2):
        for f in range(fields):
            for g in range(main):
                tiles[stat] = jnp.where(lane == f * main + g, total_of(sums[stat, f, g]), tiles[stat])
    for d in range(pay.shape[0]):
        pay[d, :GROUP, :] = tiles[0]
        pay[d, GROUP:, :] = tiles[1]


def spread_columns(tile, cols, spots):
    for i, spot in enumerate(spots):
        cols[i] = column(tile, spot, LANE)


def tiles_of(assets):
    return [pl.ds(at, LANE) for at in range(0, assets, LANE)]


def row_moments(source, mine, inverse, where, cs, ss):
    fields, _, assets = source.shape
    acc = [None] * (2 * fields)

    def added(i, x):
        acc[i] = x if acc[i] is None else acc[i] + x

    for lanes in tiles_of(assets):
        listed = inverse[where, lanes] > 0.0
        for f in range(fields):
            z = clipped_score(source[f, mine, lanes], cs[f], ss[f])
            z = jnp.where(listed, z, 0.0)
            added(f, z)
            added(fields + f, z * z)
    return acc


def group_rows(g):
    return pl.ds(pl.multiple_of(g * GROUP, GROUP), GROUP)


def second_pass(gathered, low, high, inverse, stats, part, centers, scales, sums):
    fields, _, assets = low.shape
    main = (inverse.shape[0] - LATE) // GROUP - SKIP_GROUPS
    first = fields * main
    total = summed(gathered)
    t0, t1 = total[:GROUP], total[GROUP:]
    lane = lanes_iota()
    present = t1
    for f in range(fields):
        moved = pltpu.roll(t0, (f * main - first) % LANE, 1)
        present = jnp.where((lane >= f * main) & (lane < (f + 1) * main), moved, present)
    present = jnp.maximum(present, 1.0)
    center, scale = moments(t0, t1, present)
    stats[0], stats[1], stats[2] = center, scale, present
    spread_columns(center, centers, range(first))
    spread_columns(scale, scales, range(first))

    half = main // 2
    for source, skip in ((low, 0), (high, half)):

        def group(pair, carry):
            for i in (2 * pair, 2 * pair + 1):
                g = i + skip
                cs = [centers[f * main + g] for f in range(fields)]
                ss = [scales[f * main + g] for f in range(fields)]
                where = group_rows(g + SKIP_GROUPS)
                acc = row_moments(source, group_rows(i), inverse, where, cs, ss)
                for stat in range(2):
                    for f in range(fields):
                        sums[stat, f * main + g] = acc[stat * fields + f]
            return carry

        lax.fori_loop(0, half // 2, group, 0)
    for stat in range(2):
        tile = jnp.zeros((GROUP, LANE), jnp.float32)
        for spot in range(first):
            tile = jnp.where(lane == spot, total_of(sums[stat, spot]), tile)
        part[rows_of(stat), :] = tile


def late_first_pass(edge, tail, head, from_ref, inverse, part, late, whole, pay, sums):
    fields, _, assets = edge.shape
    rows = inverse.shape[0] - LATE
    base, base_next = block_starts(rows)
    follows = jnp.where(base_next > 0, 1.0, 0.0)
    width = 4 * LANE
    sub = sublanes(width)
    lane = lanes_iota()
    first = LANE - 2 * fields * LATE_GROUPS
    tiles = [part[:GROUP, :], part[GROUP:, :]]
    for f in range(fields):

        def tile(i, acc):
            lanes = pl.ds(pl.multiple_of(i * width, width), width)
            age = sub - jnp.maximum(from_ref[:, lanes], 0)
            acc = list(acc)
            for side, ref, at in ((0, tail, base - LATE), (1, head, base_next)):
                start = age + at
                masked = [
                    jnp.where(start >= -g * GROUP, ref[f, rows_of(g), lanes], 0.0)
                    for g in range(LATE_GROUPS)
                ]
                running, last = prefix_groups(masked, width)
                if side == 0:
                    whole[f, :, lanes] = last
                for g in range(LATE_GROUPS):
                    if side == 0:
                        where = rows_of(LATE_GROUPS + g)
                        r = edge[f, where, lanes] + (last - running[g])
                    else:
                        where = rows_of(rows // GROUP + g)
                        start_rows = rows_of(SKIP_GROUPS + g)
                        r = edge[f, start_rows, lanes] * follows + running[g]
                    r = r * inverse[where, lanes]
                    late[f, rows_of(side * LATE_GROUPS + g), lanes] = r
                    k = side * LATE_GROUPS + g
                    acc[k] = acc[k] + folded(r)
                    acc[2 * LATE_GROUPS + k] = acc[2 * LATE_GROUPS + k] + folded(r * r)
            return tuple(acc)

        zero = jnp.zeros((GROUP, LANE), jnp.float32)
        acc = lax.fori_loop(0, assets // width, tile, (zero,) * (4 * LATE_GROUPS))
        for i in range(4 * LATE_GROUPS):
            sums[f, i] = acc[i]
    for f in range(fields):
        for side in range(2):
            for g in range(LATE_GROUPS):
                spot = first + (side * fields + f) * LATE_GROUPS + g
                for stat in range(2):
                    value = total_of(sums[f, (stat * 2 + side) * LATE_GROUPS + g])
                    tiles[stat] = jnp.where(lane == spot, value, tiles[stat])
    for d in range(pay.shape[0]):
        pay[d, :GROUP, :] = tiles[0]
        pay[d, GROUP:, :] = tiles[1]


def packed(t):
    half = LANE // 2
    low = pltpu.roll(t, half, 1)
    lane = lax.broadcasted_iota(jnp.int32, (GROUP // 2, LANE), 1)
    return jnp.where(lane < half, low[: GROUP // 2], t[GROUP // 2 :])


def unpacked(p):
    return jnp.concatenate([pltpu.roll(p, LANE // 2, 1), p], axis=0)


def late_second_pass(gathered, stats, late, inverse, level, pay):
    fields, _, assets = late.shape
    rows = inverse.shape[0] - LATE
    total = summed(gathered)
    center, scale = moments(total[:GROUP], total[GROUP:], stats[2])
    level[0], level[1] = center, scale
    first = LANE - 2 * fields * LATE_GROUPS
    back = LANE - first
    lane = lanes_iota()
    out = jnp.zeros((GROUP, LANE), jnp.float32)
    for side in range(2):
        for g in range(LATE_GROUPS):
            spots = [first + (side * fields + f) * LATE_GROUPS + g for f in range(fields)]
            cs = [column(center, spot, LANE) for spot in spots]
            ss = [column(scale, spot, LANE) for spot in spots]
            where = rows_of(LATE_GROUPS + g if side == 0 else rows // GROUP + g)
            mine = rows_of(side * LATE_GROUPS + g)
            acc = row_moments(late, mine, inverse, where, cs, ss)
            for f in range(fields):
                out = jnp.where(lane == spots[f], total_of(acc[f]), out)
                out = jnp.where(lane == spots[f] - back, total_of(acc[fields + f]), out)
    out = packed(out)
    for d in range(pay.shape[0]):
        pay[d] = out


def final_rows(f, where, source, mine, inverse, stage, put, cols):
    c1, s1, c2, s2 = cols
    for lanes in tiles_of(source.shape[2]):
        z = (clipped_score(source[f, mine, lanes], c1, s1) - c2) * s2
        stage[f, put, lanes] = jnp.where(inverse[where, lanes] > 0.0, z, 0.0)


def send_pass(gathered, stats, level, level4, pay):
    total = unpacked(summed(gathered))
    back = 32
    square = pltpu.roll(total, back, 1)
    center, scale = moments(total, square, stats[2])
    level4[0], level4[1] = center, scale
    lane = lanes_iota()
    out = jnp.zeros((GROUP, LANE), jnp.float32)
    for i, t in enumerate((level[0], level[1], center, scale)):
        moved = pltpu.roll(t, 16 * (i + 1), 1)
        out = jnp.where((lane >= 16 * i) & (lane < 16 * (i + 1)), moved, out)
    pay[...] = out


def final_pass(
    edge, low, high, late, tail, whole, from_ref, inverse, centers, scales, level, level4,
    out, rolled, stage, sems,
):
    fields, rows, assets = out.shape
    main = rows // GROUP - SKIP_GROUPS
    first = LANE - 2 * fields * LATE_GROUPS
    late_tiles = (level[0], level[1], level4[0], level4[1])
    copies = []
    half = main // 2
    for f in range(fields):
        for g in range(LATE_GROUPS):
            spot = first + f * LATE_GROUPS + g
            column_set = [column(t, spot, LANE) for t in late_tiles]
            where = rows_of(LATE_GROUPS + g)
            final_rows(f, where, late, rows_of(g), inverse, stage, rows_of(g), column_set)
        for part in range(2):
            for g in range(part * half, (part + 1) * half):
                spot = f * main + g
                c2, s2 = column(level[0], spot, LANE), column(level[1], spot, LANE)
                where = rows_of(g + SKIP_GROUPS)
                put = rows_of(g + LATE_GROUPS)
                column_set = (centers[spot], scales[spot], c2, s2)
                source = (low, high)[part]
                mine = rows_of(g - part * half)
                final_rows(f, where, source, mine, inverse, stage, put, column_set)
            begin = part * (LATE_GROUPS + half) * GROUP
            size = (half + (LATE_GROUPS if part == 0 else 0)) * GROUP
            copy = pltpu.make_async_copy(
                stage.at[f, pl.ds(begin, size), :],
                out.at[f, pl.ds(LATE + begin, size), :],
                sems.at[2 * f + part],
            )
            copy.start()
            copies.append(copy)
    base = block_starts(rows)[0]
    width = 4 * LANE
    sub = sublanes(width)
    for f in range(fields):

        def tile(i, carry):
            lanes = pl.ds(pl.multiple_of(i * width, width), width)
            start = sub - jnp.maximum(from_ref[:, lanes], 0) + (base - WINDOW)
            masked = [
                jnp.where(start >= -g * GROUP, tail[f, rows_of(g), lanes], 0.0)
                for g in range(LATE_GROUPS)
            ]
            running, last = prefix_groups(masked, width)
            last = last + whole[f, :, lanes]
            for g in range(LATE_GROUPS):
                r = edge[f, rows_of(g), lanes] + (last - running[g])
                rolled[f, rows_of(g), lanes] = r * inverse[rows_of(g), lanes]
            return carry

        lax.fori_loop(0, assets // width, tile, 0)
    for copy in copies:
        copy.wait()


def head_final_pass(rolled, inverse, sent, prior, out, stage, sems):
    fields, _, assets = rolled.shape
    levels = sent[...]
    copies = []
    for f in range(fields):
        for g in range(LATE_GROUPS):
            cols = [column(levels, 16 * i + f * LATE_GROUPS + g, LANE) for i in range(4)]
            rows = rows_of(g)
            final_rows(f, rows, rolled, rows, inverse, stage, rows, cols)
        copy = pltpu.make_async_copy(stage.at[f], out.at[f, pl.ds(0, LATE), :], sems.at[f])
        copy.start()
        copies.append(copy)
    for copy in copies:
        copy.wait()


def shape(*dims):
    return jax.ShapeDtypeStruct(dims, jnp.float32)


def call(body, name, ins, outs, out_specs, scratch=(), limit=8, flops=0, aliases=None):
    return pl.pallas_call(
        body,
        name=name,
        out_shape=outs,
        in_specs=ins,
        out_specs=out_specs,
        scratch_shapes=list(scratch),
        input_output_aliases=aliases or {},
        compiler_params=pltpu.CompilerParams(vmem_limit_bytes=limit * MIB),
        cost_estimate=pl.CostEstimate(flops=flops, bytes_accessed=0, transcendentals=0),
    )


def per_device(values, listed_from, listed_until):
    fields, rows, assets = values.shape
    n = lax.axis_size("asset")
    blocks = lax.axis_size("tm")
    ring = [(i, (i + 1) % blocks) for i in range(blocks)]
    back = [((i + 1) % blocks, i) for i in range(blocks)]
    work = fields * rows * assets
    slab = shape(fields, LATE, assets)
    near, head = call(
        cut, "cut", [HBM], (slab, slab), (VMEM, VMEM), [pltpu.SemaphoreType.DMA((2,))],
        limit=44,
    )(values)
    tail_near = lax.ppermute(near, "tm", ring)
    head = lax.ppermute(head, "tm", back)
    opened, closed = listed_from.reshape(1, assets), listed_until.reshape(1, assets)
    main = rows // GROUP - SKIP_GROUPS
    tile = shape(GROUP, LANE)
    pair = shape(2, GROUP, LANE)
    exchange = functools.partial(
        lax.all_to_all, axis_name="asset", split_axis=0, concat_axis=0, tiled=True
    )

    width = 2 * LANE
    chunks = assets // width
    half = shape(fields, (rows - WINDOW) // 2, assets)
    edge, low, high, inverse, pay, far = call(
        first_pass, "first_pass", [HBM] * 3,
        (
            shape(fields, WINDOW + LATE, assets), half, half,
            shape(rows + LATE, assets), shape(n, 2 * GROUP, LANE), slab,
        ),
        (VMEM,) * 6,
        [
            pltpu.VMEM((1, assets), jnp.int32),
            pltpu.VMEM((1, assets), jnp.int32),
            pltpu.VMEM((chunks, fields, rows, width), jnp.float32),
            pltpu.VMEM((2, fields, main, GROUP, LANE), jnp.float32),
            pltpu.SemaphoreType.DMA((chunks,)),
            pltpu.SemaphoreType.DMA((2,)),
        ],
        limit=40, flops=20 * work,
    )(values, opened, closed)
    gathered = exchange(pay)
    columns = shape(fields * main, GROUP, LANE)
    stats, part, centers, scales = call(
        second_pass, "second_pass", [VMEM] * 4,
        (shape(3, GROUP, LANE), shape(2 * GROUP, LANE), columns, columns), (VMEM,) * 4,
        [pltpu.VMEM((2, fields * main, GROUP, LANE), jnp.float32)], limit=16, flops=10 * work,
    )(gathered, low, high, inverse)
    far, part = lax.optimization_barrier((far, part))
    tail_far = lax.ppermute(far, "tm", ring)
    late, whole, pay = call(
        late_first_pass, "late_first_pass", [VMEM] * 6,
        (shape(fields, 2 * LATE, assets), shape(fields, GROUP, assets), shape(n, 2 * GROUP, LANE)),
        (VMEM, VMEM, VMEM),
        [pltpu.VMEM((fields, 4 * LATE_GROUPS, GROUP, LANE), jnp.float32)], limit=20, flops=5 * work,
    )(edge, tail_near, head, opened, inverse, part)
    gathered = exchange(pay)
    level, pay = call(
        late_second_pass, "late_second_pass", [VMEM] * 4,
        (pair, shape(n, GROUP // 2, LANE)), (VMEM, VMEM), limit=16, flops=3 * work,
    )(gathered, stats, late, inverse)
    gathered = exchange(pay)
    level4, pay = call(
        send_pass, "send_pass", [VMEM] * 3, (pair, tile), (VMEM, VMEM), flops=work // 100,
    )(gathered, stats, level)
    sent = lax.ppermute(pay, "tm", ring)
    out, rolled = call(
        final_pass, "final_pass", [VMEM] * 12,
        (shape(fields, rows, assets), slab), (HBM, VMEM),
        [
            pltpu.VMEM((fields, rows - LATE, assets), jnp.float32),
            pltpu.SemaphoreType.DMA((2 * fields,)),
        ],
        limit=16, flops=10 * work,
    )(edge, low, high, late, tail_far, whole, opened, inverse, centers, scales, level, level4)
    return call(
        head_final_pass, "head_final_pass", [VMEM] * 3 + [HBM],
        shape(fields, rows, assets), HBM,
        [pltpu.VMEM((fields, LATE, assets), jnp.float32), pltpu.SemaphoreType.DMA((fields,))],
        limit=16, flops=2 * work, aliases={3: 0},
    )(rolled, inverse, sent, out)


def solution(mesh):
    in_specs = (P(None, "tm", "asset"), P("asset"), P("asset"))
    out_specs = P(None, "tm", "asset")
    return jax.shard_map(
        per_device, mesh=mesh, in_specs=in_specs, out_specs=out_specs, check_vma=False
    )
```
